128 devices in a mesh: tm: 2 (over core), stn: 8 (over y_hi, z), chan: 8 (over x, y_lo).
Axes of the slice: x: 4, y: 4 (y_hi: 2, y_lo: 2; y = y_hi * 2 + y_lo), z: 4, core: 2. Of those that a mesh axis runs over, the one named last changes fastest.
Arguments:
- voltages: bfloat16 [2, 8, 512, 32, 2, 256], P(None, 'chan', 'stn', 'tm'), may hold values from -100 to 100
- fir_taps: float32 [16, 256], replicated, may hold values from -1.5 to 1.5
- station_map: int32 [512], P('stn'), may hold values from 0 to 31, as said below
- beam_index: int32 [512], P('stn'), may hold values from 0 to 15
- weight_table: bfloat16 [2, 16, 8, 8], P(None, None, 'chan'), may hold values from -1.5 to 1.5
Outputs:
- visibilities: float32 [2, 2, 8, 32, 32, 8, 2, 2, 256], P('tm', None, 'chan', 'stn')
The draws below stay inside these ranges and needn't reach their ends.
Inputs may be any that keep to these rules, and one draw needn't show every extreme that they name: `station_map`: each station number names exactly 16 dishes; of the dishes g * 64 up to (g + 1) * 64 - 1, exactly 8 name a station of the block h * 4 up to (h + 1) * 4 - 1, for every g and h.
All inputs are finite; a program needn't handle non-finite values.
Results may differ from the reference program's by a relative error of at most 0.017.
Values may be sent and summed in bfloat16 or wider, within the bound.
A program may use at most 512 MiB of HBM per device.

```python
import jax
import jax.numpy as jnp
from jax import lax

DISHES = 512
STATIONS = 32
DPS = 16
BEAMS = 8
POL = 2
COARSE = 8
FINE = 256
TAPS = 16
NTAB = 16
FRAMES_DEV = 16
FRAMES = 32
N_TM = 2
N_STN = 8


def draw_voltages(key, part):
    noise_key, sample_key, frame_key = jax.random.split(jax.random.fold_in(key, 11), 3)
    shape = (2, COARSE, DISHES, FRAMES, POL, FINE)
    noise_draw = jnp.clip(jax.random.normal(noise_key, shape, jnp.float32), -6.0, 6.0)
    rise_factor = 3.0
    coarse_pos = jnp.arange(COARSE, dtype=jnp.float32) / max(COARSE - 1, 1)
    coarse_amp = jnp.sqrt(rise_factor ** coarse_pos)
    sample_amp = 10.0 ** (0.5 * jax.random.uniform(sample_key, (FINE,), jnp.float32))
    frame_amp = 3.0 ** (0.5 * jax.random.uniform(frame_key, (FRAMES,), jnp.float32))
    scaled = noise_draw * coarse_amp[None, :, None, None, None, None] * frame_amp[None, None, None, :, None, None] * sample_amp
    return scaled.astype(jnp.bfloat16)


def draw_station_map(key, part):
    group_dishes = DISHES // N_STN
    share = group_dishes // N_STN
    owned = STATIONS // N_STN
    first_key, second_key = jax.random.split(jax.random.fold_in(key, 23), 2)
    base = jnp.arange(group_dishes, dtype=jnp.int32)
    ranks = jax.vmap(lambda sub_key: jax.random.permutation(sub_key, base))(jax.random.split(first_key, N_STN))
    placing = jax.vmap(lambda sub_key: jax.random.permutation(sub_key, base))(jax.random.split(second_key, N_STN))
    owner = ranks // share
    group_ids = jnp.arange(N_STN, dtype=jnp.int32)[:, None]
    column = group_ids * share + ranks % share
    position = placing[owner, column]
    station = owner * owned + position // (DISHES // STATIONS)
    return station.reshape(DISHES).astype(jnp.int32)


def place_ends(values, stream_key, least, largest):
    dims = values.shape
    index_at = [jax.random.randint(jax.random.fold_in(stream_key, axis), (), 0, dims[axis]) for axis in range(len(dims))]
    values = values.at[tuple(index_at)].set(least)
    longest = dims.index(max(dims))
    index_at[longest] = (index_at[longest] + 1) % dims[longest]
    return values.at[tuple(index_at)].set(largest)


def level_of(key, shape, cuts, smallest, largest):
    def one(dim, blocks):
        heights = jax.random.uniform(jax.random.fold_in(jax.random.fold_in(key, 6), dim), (blocks,), jnp.float32, smallest / len(cuts), largest / len(cuts))
        return jnp.repeat(jnp.exp(heights), shape[dim] // blocks).reshape((-1,) + (1,) * (len(shape) - dim - 1))

    level = one(*cuts[0])
    for cut in cuts[1:]:
        level = level * one(*cut)
    return level


def bell_draw(rng, shape, deviation, most, pieces=(), kind=jnp.bfloat16):
    level = level_of(rng, shape, pieces, -0.22, 0.18) if pieces else 1.0
    array = jax.random.normal(rng, shape, jnp.float32) * deviation * level
    return jnp.minimum(jnp.maximum(array, -most), most).astype(kind)


def setup_inputs(seed: int = 0) -> dict:
    seeds = jax.random.split(jax.random.key(seed), 6)
    voltages = draw_voltages(jax.random.fold_in(seeds[5], 71), 0)
    fir_taps = bell_draw(seeds[1], (TAPS, FINE), TAPS ** -0.5, 1.5, (), jnp.float32)
    station_map = draw_station_map(jax.random.fold_in(seeds[5], 71), 0)
    beam_index = place_ends(jax.random.randint(seeds[3], (DISHES,), 0, NTAB), jax.random.fold_in(seeds[3], 1), 0, NTAB - 1).astype(jnp.int32)
    weight_table = bell_draw(seeds[4], (2, NTAB, COARSE, BEAMS), DPS ** -0.5, 1.5, ((2, 8),))
    return {"voltages": voltages, "fir_taps": fir_taps, "station_map": station_map, "beam_index": beam_index, "weight_table": weight_table}


epsilon = 1e-06

def dft_tables(length):
    bin_index = jnp.arange(length, dtype=jnp.int32)
    phase_step = bin_index[:, None] * bin_index[None, :] % length
    angles = phase_step.astype(jnp.float32) * (2.0 * jnp.pi / length)
    return (jnp.cos(angles).astype(jnp.bfloat16), jnp.sin(angles).astype(jnp.bfloat16))

def correlate(normed_slice):
    values = normed_slice.astype(jnp.float32)
    real_part = values[:, 0]
    imag_part = values[:, 1]

    def product(left_beams, right_beams):
        return jnp.einsum('sbfpk,tbfqk->stbpqk', left_beams, right_beams)
    vis_re = product(real_part, real_part) + product(imag_part, imag_part)
    vis_im = product(imag_part, real_part) - product(real_part, imag_part)
    return jnp.stack([vis_re, vis_im]) / FRAMES_DEV

def reference(voltages, fir_taps, station_map, beam_index, weight_table):
    cosine, sine_table = dft_tables(FINE)
    history = TAPS - 1
    group_size = DISHES // N_STN
    station_hot = (station_map[:, None] == jnp.arange(STATIONS, dtype=jnp.int32)[None, :]).astype(jnp.float32)
    table_hot = (beam_index[:, None] == jnp.arange(NTAB, dtype=jnp.int32)[None, :]).astype(jnp.float32)

    def channel_beams(inputs):
        samples, table_slice = inputs
        padded = jnp.pad(samples, ((0, 0), (0, 0), (history, 0), (0, 0), (0, 0)))
        filtered = jnp.zeros(samples.shape, jnp.float32)
        for tap_index in range(TAPS):
            offset = history - tap_index
            filtered = filtered + fir_taps[tap_index] * padded[:, :, offset:offset + FRAMES].astype(jnp.float32)
        filtered = filtered.astype(jnp.bfloat16)
        real_part = filtered[0].reshape(-1, FINE)
        imag_part = filtered[1].reshape(-1, FINE)
        spec_re = jnp.dot(real_part, cosine, preferred_element_type=jnp.float32) + jnp.dot(imag_part, sine_table, preferred_element_type=jnp.float32)
        spec_im = jnp.dot(imag_part, cosine, preferred_element_type=jnp.float32) - jnp.dot(real_part, sine_table, preferred_element_type=jnp.float32)
        spectra_low = jnp.stack([spec_re, spec_im]).reshape(samples.shape).astype(jnp.bfloat16)
        spectra = lax.optimization_barrier(spectra_low).astype(jnp.float32)
        weights = jnp.einsum('dt,otb->odb', table_hot, table_slice.astype(jnp.float32))
        weight_re = weights[0]
        weight_im = weights[1]
        mixing = jnp.stack([jnp.stack([weight_re, -weight_im]), jnp.stack([weight_im, weight_re])])
        steering = station_hot[None, None, :, :, None] * mixing[:, :, :, None, :]
        summed = jnp.zeros((STATIONS, 2, BEAMS, FRAMES, POL, FINE), jnp.float32)
        for dish_group in range(N_STN):
            low_dish = dish_group * group_size
            partial_value = jnp.einsum('oidsb,idfpk->sobfpk', steering[:, :, low_dish:low_dish + group_size], spectra[:, low_dish:low_dish + group_size])
            rounded = lax.optimization_barrier(partial_value.astype(jnp.bfloat16))
            summed = summed + rounded.astype(jnp.float32)
        return summed.astype(jnp.bfloat16)
    formed = lax.map(channel_beams, (jnp.moveaxis(voltages, 1, 0), jnp.moveaxis(weight_table, 2, 0)))
    outputs = []
    for time_block in range(N_TM):
        first_frame = time_block * FRAMES_DEV
        values = formed[:, :, :, :, first_frame:first_frame + FRAMES_DEV].astype(jnp.float32)
        power_sum = lax.optimization_barrier(jnp.sum(values * values, axis=(0, 2, 4, 6)))
        inverse_rms = lax.rsqrt(power_sum / (COARSE * FRAMES_DEV * FINE) + epsilon)
        normed = (values * inverse_rms[None, :, None, :, None, :, None]).astype(jnp.bfloat16)
        visibility = lax.map(correlate, normed)
        outputs.append(jnp.moveaxis(visibility, 0, 1))
    return jnp.stack(outputs)
```

```python
import functools

import jax
import jax.numpy as jnp
import numpy as np
from jax import lax
from jax.experimental import pallas as pl
from jax.experimental.pallas import tpu as pltpu
from jax.sharding import PartitionSpec as P

MESH = pl.DeviceIdType.MESH
F32 = jnp.float32
BF16 = jnp.bfloat16
EPSILON = 1e-06
STN = 8
RING = 4
CHAN = 8
SHARE = 8
OWN = 4
BEAMS = 8
POL = 2
FRAMES = 16
TAPS = 16
FINE = 256
LANES = 128
NT = FINE // LANES
HISTORY = TAPS - 1
PITCH = 72
DENOMINATOR = float(CHAN * FRAMES * FINE)


def dft_table():
    step = np.arange(FINE)
    angle = (step[:, None] * step[None, :] % FINE) * (2.0 * np.pi / FINE)
    cosine, sine = np.cos(angle), np.sin(angle)
    return np.block([[cosine, -sine], [sine, cosine]]).astype(np.float32)


def kernel(
    perm_ref, v_ref, wt_ref, taps_ref, tab_ref, out_ref,
    regroup, send_v, recv_v, recv_wt, weights, beams, filtered, formed, scaled, stage, packed,
    power, power_all, inverse,
    a_send, a_recv, w_send, w_recv, h_send, h_recv, g_send, g_recv, f_send,
    p_send, p_recv, i_send, i_recv, o_sem, x_send, x_recv,
):
    half = lax.axis_index("tm")
    me = lax.axis_index("stn")
    chan = lax.axis_index("chan")
    row, col = me // RING, me % RING
    up = row * RING + lax.rem(col + 1, RING)
    down = row * RING + lax.rem(col + 3, RING)
    far = row * RING + lax.rem(col + 2, RING)
    pair = (1 - row) * RING + col
    peers = {1: up, 2: far, 3: down, 4: pair}

    def remote(src, dst, send, recv, **where):
        return pltpu.make_async_remote_copy(
            src_ref=src, dst_ref=dst, send_sem=send, recv_sem=recv,
            device_id=where, device_id_type=MESH,
        )

    barrier = pltpu.get_barrier_semaphore()
    pl.semaphore_signal(barrier, inc=1, device_id={"tm": 1 - half}, device_id_type=MESH)
    for step in range(1, STN):
        pl.semaphore_signal(
            barrier, inc=1, device_id={"stn": lax.rem(me + step, STN)}, device_id_type=MESH
        )
    for step in range(1, CHAN):
        pl.semaphore_signal(
            barrier, inc=1, device_id={"chan": lax.rem(chan + step, CHAN)}, device_id_type=MESH
        )

    def regrouped(step, store):
        holder = lax.rem(me + step, STN)
        for part in range(2):
            for e in range(SHARE):
                dish = perm_ref[holder * SHARE + e]
                line = (part * SHARE + e) * PITCH
                regroup[line : line + FRAMES * NT * POL, :] = v_ref[part, dish].astype(F32)
        for pol in range(POL):
            for tile in range(FRAMES * NT):
                value = regroup[pl.ds(tile * POL + pol, 2 * SHARE, stride=PITCH), :]
                store(pol, tile * LANES, value.astype(BF16))

    mine = pl.ds(pl.multiple_of(me * 2 * SHARE, 2 * SHARE), 2 * SHARE)

    def dish_copy(pol, step):
        return remote(
            send_v.at[step - 1, pol], recv_v.at[pol, mine],
            a_send.at[pol, step - 1], a_recv.at[pol, step - 1], stn=lax.rem(me + step, STN),
        )

    def weight_copy(step):
        holder = lax.rem(me + step, STN)
        return remote(
            wt_ref.at[holder], recv_wt.at[mine], w_send.at[step - 1], w_recv.at[step - 1], stn=holder
        )

    def prepare(step, carry):
        def store(pol, lane, value):
            send_v[step - 1, pol, :, lane : lane + LANES] = value

        regrouped(step, store)
        return carry

    def prepare_and_send(step, carry):
        prepare(step, carry)
        dish_copy(0, step - 1).start()
        return carry

    prepare(1, 0)
    pl.semaphore_wait(barrier, 1 + (STN - 1) + (CHAN - 1))
    for step in range(1, STN):
        weight_copy(step).start()
    lax.fori_loop(2, STN, prepare_and_send, 0)

    def store_own(pol, lane, value):
        recv_v[pol, mine, lane : lane + LANES] = value

    regrouped(0, store_own)
    dish_copy(0, STN - 1).start()
    lax.fori_loop(1, STN, lambda step, c: (dish_copy(1, step).start(), c)[1], 0)
    recv_wt[mine, :] = wt_ref[me]
    power[...] = jnp.zeros_like(power)
    lane_id = lax.broadcasted_iota(jnp.int32, (BEAMS, LANES), 1)

    for step in range(1, STN):
        weight_copy(step).wait_recv()
    weights[...] = jnp.transpose(recv_wt[...].astype(F32))[: 2 * OWN * BEAMS, :].astype(BF16)

    def halo_copy(pol):
        return remote(
            beams.at[pol, :, pl.ds((HISTORY + 1) * BEAMS, HISTORY * BEAMS), :],
            beams.at[pol, :, pl.ds(0, HISTORY * BEAMS), :],
            h_send.at[pol], h_recv.at[pol], tm=1 - half,
        )

    def chunk_copies(chunk):
        own = formed.at[0, chunk]
        return (
            remote(own, formed.at[3, chunk], g_send.at[0, chunk], g_recv.at[3, chunk], stn=up),
            remote(own, formed.at[1, chunk], g_send.at[1, chunk], g_recv.at[1, chunk], stn=down),
            remote(own, formed.at[4, chunk], g_send.at[2, chunk], g_recv.at[4, chunk], stn=pair),
        )

    for pol in range(POL):
        lax.fori_loop(1, STN, lambda step, c: (dish_copy(pol, step).wait_recv(), c)[1], 0)

        def steer(frame, carry):
            lanes = pl.ds(pl.multiple_of(frame * FINE, FINE), FINE)
            value = jnp.dot(weights[...], recv_v[pol, :, lanes], preferred_element_type=F32)
            line = pl.ds(pl.multiple_of((HISTORY + frame) * BEAMS, BEAMS), BEAMS)
            for j in range(2 * OWN):
                beams[pol, j, line, :] = value[j * BEAMS : (j + 1) * BEAMS, :]
            return carry

        lax.fori_loop(0, FRAMES, steer, 0)

        @pl.when(half == 0)
        def _():
            beams[pol, :, : HISTORY * BEAMS, :] = jnp.zeros((2 * OWN, HISTORY * BEAMS, FINE), F32)
            halo_copy(pol).start()

        @pl.when(half == 1)
        def _():
            halo_copy(pol).wait_recv()

        def filter_station(station, carry):
            for part in range(2):
                for tile in range(NT):
                    lanes = slice(tile * LANES, (tile + 1) * LANES)
                    taps = [
                        jnp.broadcast_to(taps_ref[j : j + 1, lanes], (BEAMS, LANES))
                        for j in range(TAPS)
                    ]
                    outs = []
                    for frame in range(FRAMES):
                        total = None
                        for j in range(TAPS):
                            line = (frame + HISTORY - j) * BEAMS
                            term = taps[j] * beams[
                                pol, part * OWN + station, line : line + BEAMS, lanes
                            ]
                            total = term if total is None else total + term
                        outs.append(total)
                        if frame % 2:
                            base = pl.multiple_of(
                                station * FRAMES * BEAMS + (frame - 1) * BEAMS, 2 * BEAMS
                            )
                            lane = part * FINE + tile * LANES
                            filtered[pl.ds(base, 2 * BEAMS), lane : lane + LANES] = (
                                jnp.concatenate(outs, axis=0).astype(BF16)
                            )
                            outs = []
            return carry

        lax.fori_loop(0, OWN, filter_station, 0)

        def transform(station, carry):
            lines = pl.ds(pl.multiple_of(station * FRAMES * BEAMS, FRAMES * BEAMS), FRAMES * BEAMS)
            value = jnp.dot(filtered[lines, :], tab_ref[...], preferred_element_type=F32)
            formed[0, pol * OWN + station] = value.astype(BF16)
            squares = jnp.sum((value * value).reshape(FRAMES, BEAMS, 2 * FINE), axis=0)
            squares = sum(squares[:, k * LANES : (k + 1) * LANES] for k in range(4))
            total = jnp.sum(squares, axis=1, keepdims=True)
            power[...] += jnp.where(lane_id == station * POL + pol, total, 0.0)
            return carry

        lax.fori_loop(0, OWN, transform, 0)

        def send_chunk(station, carry):
            for copy in chunk_copies(pol * OWN + station):
                copy.start()
            return carry

        lax.fori_loop(0, OWN, send_chunk, 0)

    def power_copy(step):
        return remote(
            power, power_all.at[step - 1], p_send.at[step - 1], p_recv.at[step - 1],
            chan=lax.rem(chan + step, CHAN),
        )

    for step in range(1, CHAN):
        power_copy(step).start()
    for step in range(1, CHAN):
        power_copy(step).wait_recv()
    total = power[...]
    for step in range(1, CHAN):
        total = total + power_all[step - 1]
    inverse[0] = lax.rsqrt(total / DENOMINATOR + EPSILON)
    inverse_copies = [
        remote(inverse.at[0], inverse.at[slot], i_send.at[slot], i_recv.at[slot], stn=target)
        for slot, target in ((1, down), (2, far), (3, up), (4, pair))
    ]

    def lane_of(slot, index):
        tile = inverse[slot]
        one = jnp.sum(jnp.where(lane_id == index, tile, 0.0), axis=1, keepdims=True)
        return jnp.broadcast_to(one, (BEAMS, LANES))

    def scale_chunk(which, slot, station):
        for pol in range(POL):
            factor = lane_of(slot, station * POL + pol) * (1.0 / FRAMES)
            for pairs in range(FRAMES // 2):
                lines = slice(pairs * 2 * BEAMS, (pairs + 1) * 2 * BEAMS)
                for tile in range(4):
                    lanes = slice(tile * LANES, (tile + 1) * LANES)
                    value = formed[slot, pol * OWN + station, lines, lanes].astype(F32)
                    scaled[which, station * POL + pol, lines, lanes] = jnp.concatenate(
                        [value[:BEAMS] * factor, value[BEAMS:] * factor], axis=0
                    )

    def correlate(which, slot, station, unit, swapped):
        for q in range(POL):
            factor = lane_of(slot, station * POL + q)
            for tile in range(NT):
                re_lanes = slice(tile * LANES, (tile + 1) * LANES)
                im_lanes = slice(FINE + tile * LANES, FINE + (tile + 1) * LANES)
                real = [None] * (OWN * POL)
                imag = [None] * (OWN * POL)
                for pairs in range(FRAMES // 2):
                    lines = slice(pairs * 2 * BEAMS, (pairs + 1) * 2 * BEAMS)
                    right_re = formed[slot, q * OWN + station, lines, re_lanes].astype(F32)
                    right_im = formed[slot, q * OWN + station, lines, im_lanes].astype(F32)
                    for part in range(2):
                        cr = right_re[part * BEAMS : (part + 1) * BEAMS]
                        ci = right_im[part * BEAMS : (part + 1) * BEAMS]
                        line = (pairs * 2 + part) * BEAMS
                        for c in range(OWN * POL):
                            ar = scaled[which, c, line : line + BEAMS, re_lanes]
                            ai = scaled[which, c, line : line + BEAMS, im_lanes]
                            re = ar * cr + ai * ci
                            im = ar * ci - ai * cr if swapped else ai * cr - ar * ci
                            real[c] = re if real[c] is None else real[c] + re
                            imag[c] = im if imag[c] is None else imag[c] + im
                for c in range(OWN * POL):
                    s, p = c // POL, c % POL
                    line = q * 4 + tile * 2 + p if swapped else p * 4 + tile * 2 + q
                    lines = pl.ds(line, BEAMS, stride=8)
                    stage[0, s, lines, :] = real[c] * factor
                    stage[1, s, lines, :] = imag[c] * factor
        packed[unit] = stage[...].astype(BF16)

    def out_copy(unit, block, station):
        return pltpu.make_async_copy(
            packed.at[unit], out_ref.at[:, :, block * OWN + station], o_sem.at[unit]
        )

    def arrived(slot, chunk):
        remote(
            formed.at[slot, chunk], formed.at[slot, chunk], g_send.at[0, chunk],
            g_recv.at[slot, chunk], stn=up,
        ).wait_recv()

    def forward_up(station):
        return remote(
            formed.at[3, station], formed.at[2, station],
            f_send.at[0, station], g_recv.at[2, station], stn=up,
        )

    def forward_down(station):
        chunk = OWN + station
        return remote(
            formed.at[1, chunk], formed.at[2, chunk],
            f_send.at[1, station], g_recv.at[2, chunk], stn=down,
        )

    for copy in inverse_copies:
        copy.start()

    def own_scale(station, carry):
        scale_chunk(0, 0, station)
        return carry

    lax.fori_loop(0, OWN, own_scale, 0)

    def pass_on(station, carry):
        arrived(3, station)
        forward_up(station).start()
        arrived(1, station)
        arrived(4, station)
        return carry

    def own_pairs(station, carry):
        pass_on(station, carry)
        correlate(0, 0, station, station, False)
        out_copy(station, me, station).start()
        return carry

    lax.fori_loop(0, OWN, own_pairs, 0)
    for copy in inverse_copies:
        copy.wait_recv()

    def near_pairs(station, carry):
        chunk = OWN + station
        arrived(1, chunk)
        forward_down(station).start()
        arrived(3, chunk)
        arrived(4, chunk)
        scale_chunk(1, 4, station)
        for n, slot in enumerate((1, 3, 4)):
            unit = OWN * (1 + n) + station
            correlate(0, slot, station, unit, False)
            out_copy(unit, peers[slot], station).start()
        return carry

    lax.fori_loop(0, OWN, near_pairs, 0)

    theirs = pl.ds(pl.multiple_of(pair * OWN, OWN), OWN)

    def swap_copy(n, station):
        return remote(
            packed.at[5 * OWN + n * OWN + station], out_ref.at[:, station, theirs],
            x_send.at[n, station], x_recv.at[n, station], stn=(up, down)[n],
        )

    def far_copy(station):
        return remote(
            packed.at[7 * OWN + station], out_ref.at[:, :, far * OWN + station],
            x_send.at[2, station], x_recv.at[2, station], stn=pair,
        )

    def swapped_pairs(station, carry):
        for n, slot in enumerate((1, 3)):
            correlate(1, slot, station, 5 * OWN + n * OWN + station, True)
            swap_copy(n, station).start()
        return carry

    lax.fori_loop(0, OWN, swapped_pairs, 0)

    def far_pairs(station, carry):
        arrived(2, station)
        arrived(2, OWN + station)
        correlate(1, 2, station, 7 * OWN + station, False)
        far_copy(station).start()
        correlate(0, 2, station, 4 * OWN + station, False)
        out_copy(4 * OWN + station, far, station).start()
        return carry

    lax.fori_loop(0, OWN, far_pairs, 0)

    def finish(station, carry):
        for n in range(2):
            swap_copy(n, station).wait()
        far_copy(station).wait()
        forward_up(station).wait_send()
        forward_down(station).wait_send()
        out_copy(station, me, station).wait()
        for n, slot in enumerate((1, 3, 4)):
            out_copy(OWN * (1 + n) + station, peers[slot], station).wait()
        out_copy(4 * OWN + station, far, station).wait()
        for pol in range(POL):
            for copy in chunk_copies(pol * OWN + station):
                copy.wait_send()
        return carry

    lax.fori_loop(0, OWN, finish, 0)

    def finish_sends(step, carry):
        dish_copy(0, step).wait_send()
        dish_copy(1, step).wait_send()
        weight_copy(step).wait_send()
        power_copy(step).wait_send()
        return carry

    lax.fori_loop(1, STN, finish_sends, 0)
    for copy in inverse_copies:
        copy.wait_send()

    @pl.when(half == 0)
    def _():
        for pol in range(POL):
            halo_copy(pol).wait_send()


def dish_order(station_map, beam_index, weight_table):
    dishes = station_map.shape[0]
    index = jnp.arange(dishes, dtype=jnp.int32)
    holder = station_map // OWN
    same = (holder[:, None] == holder[None, :]) & (index[None, :] < index[:, None])
    slot = holder * SHARE + jnp.sum(same.astype(jnp.int32), axis=1)
    hot = slot[None, :] == index[:, None]
    perm = jnp.sum(jnp.where(hot, index[None, :], 0), axis=1)
    station = jnp.sum(jnp.where(hot, (station_map % OWN)[None, :], 0), axis=1)
    table_row = jnp.sum(jnp.where(hot, beam_index[None, :], 0), axis=1)
    weight_re, weight_im = weight_table[0, :, 0, :], weight_table[1, :, 0, :]
    table = jnp.stack(
        [jnp.stack([weight_re, weight_im]), jnp.stack([-weight_im, weight_re])]
    )
    rows = table.shape[2]
    row_hot = table_row[:, None] == jnp.arange(rows, dtype=jnp.int32)[None, :]
    chosen = jnp.sum(
        jnp.where(row_hot[:, None, None, :, None], table[None].astype(F32), 0.0), axis=3
    )
    own_hot = station[:, None] == jnp.arange(OWN, dtype=jnp.int32)[None, :]
    steer = jnp.where(own_hot[:, None, None, :, None], chosen[:, :, :, None, :], 0.0)
    steer = steer.reshape(STN, SHARE, 2, 2 * OWN * BEAMS).swapaxes(1, 2)
    steer = steer.reshape(STN, 2 * SHARE, 2 * OWN * BEAMS)
    steer = jnp.pad(steer, ((0, 0), (0, 0), (0, LANES - 2 * OWN * BEAMS)))
    return perm.astype(jnp.int32), steer.astype(BF16)


def per_device(voltages, fir_taps, station_map, beam_index, weight_table):
    perm, steer = dish_order(station_map, beam_index, weight_table)
    parts, _, dishes, frames, pols, fine = voltages.shape
    rows = voltages.reshape(parts, dishes, frames, pols, NT, LANES)
    rows = rows.swapaxes(3, 4).reshape(parts, dishes, frames * NT * pols, LANES)
    table = jnp.asarray(dft_table(), BF16)
    vmem = pl.BlockSpec(memory_space=pltpu.VMEM)
    dma = pltpu.SemaphoreType.DMA
    chunk = (FRAMES * BEAMS, 2 * FINE)
    units = 8 * OWN
    result = pl.pallas_call(
        kernel,
        out_shape=jax.ShapeDtypeStruct((2, OWN, STN * OWN, 8 * BEAMS, LANES), BF16),
        in_specs=[pl.BlockSpec(memory_space=pltpu.SMEM)] + [vmem] * 4,
        out_specs=pl.BlockSpec(memory_space=pl.ANY),
        scratch_shapes=[
            pltpu.VMEM((2 * SHARE * PITCH, LANES), F32),
            pltpu.VMEM((STN - 1, POL, 2 * SHARE, FRAMES * FINE), BF16),
            pltpu.VMEM((POL, STN * 2 * SHARE, FRAMES * FINE), BF16),
            pltpu.VMEM((STN * 2 * SHARE, LANES), BF16),
            pltpu.VMEM((2 * OWN * BEAMS, STN * 2 * SHARE), BF16),
            pltpu.VMEM((POL, 2 * OWN, (HISTORY + FRAMES) * BEAMS, FINE), F32),
            pltpu.VMEM((OWN * FRAMES * BEAMS, 2 * FINE), BF16),
            pltpu.VMEM((5, POL * OWN, *chunk), BF16),
            pltpu.VMEM((2, OWN * POL, *chunk), F32),
            pltpu.VMEM((2, OWN, 8 * BEAMS, LANES), F32),
            pltpu.VMEM((units, 2, OWN, 8 * BEAMS, LANES), BF16),
            pltpu.VMEM((BEAMS, LANES), F32),
            pltpu.VMEM((CHAN - 1, BEAMS, LANES), F32),
            pltpu.VMEM((5, BEAMS, LANES), F32),
            dma((POL, STN - 1)), dma((POL, STN - 1)),
            dma((STN - 1,)), dma((STN - 1,)),
            dma((POL,)), dma((POL,)),
            dma((3, POL * OWN)), dma((5, POL * OWN)), dma((2, OWN)),
            dma((CHAN - 1,)), dma((CHAN - 1,)),
            dma((5,)), dma((5,)),
            dma((5 * OWN,)),
            dma((3, OWN)), dma((3, OWN)),
        ],
        compiler_params=pltpu.CompilerParams(
            collective_id=0, has_side_effects=True, vmem_limit_bytes=48 * 1024 * 1024
        ),
    )(perm, rows, steer, fir_taps, table)
    result = result.reshape(2, OWN, STN * OWN, BEAMS, POL, NT, POL, LANES)
    result = result.swapaxes(5, 6).reshape(2, 1, OWN, STN * OWN, BEAMS, POL, POL, fine)
    return result.astype(F32)[None]


def solution(mesh):
    in_specs = (
        P(None, "chan", "stn", "tm", None, None),
        P(),
        P("stn"),
        P("stn"),
        P(None, None, "chan", None),
    )
    out_specs = P("tm", None, "chan", "stn", None, None, None, None, None)
    return jax.shard_map(
        per_device, mesh=mesh, in_specs=in_specs, out_specs=out_specs, check_vma=False
    )
```

```python
import functools

import jax
import jax.numpy as jnp
import numpy as np
from jax import lax
from jax.experimental import pallas as pl
from jax.experimental.pallas import tpu as pltpu
from jax.sharding import PartitionSpec as P

MESH = pl.DeviceIdType.MESH
F32 = jnp.float32
BF16 = jnp.bfloat16
EPSILON = 1e-06
STN = 8
RING = 4
CHAN = 8
SHARE = 8
OWN = 4
HALF = OWN // 2
BEAMS = 8
POL = 2
FRAMES = 16
TAPS = 16
FINE = 256
LANES = 128
NT = FINE // LANES
HISTORY = TAPS - 1
VMEM_GRANT = 67043328 - 4 * 1024 * 1024
PITCH = 72
DENOMINATOR = float(CHAN * FRAMES * FINE)


WIDEN_STEPS = 16
WIDEN_GRANT = 62 * 1024 * 1024
ROUTE = ((1, 0), (0, 1), (0, 3), (1, 1), (1, 3), (0, 2), (1, 2))


def dft_table():
    step = np.arange(FINE)
    angle = (step[:, None] * step[None, :] % FINE) * (2.0 * np.pi / FINE)
    cosine, sine = np.cos(angle), np.sin(angle)
    return np.block([[cosine, -sine], [sine, cosine]]).astype(np.float32)


def kernel(
    perm_ref, map_hbm, row_hbm, table_hbm, v_hbm, taps_hbm, tab_hbm, out_ref,
    map_ref, row_ref, table_ref, v_ref, taps_ref, tab_ref, wt_ref, regroup, send_v, recv_v, recv_wt, weights, beams, filtered, formed, scaled, stage, packed, land_swap, land_far,
    power, power_all, inverse,
    a_send, a_recv, w_send, w_recv, h_send, h_recv, g_send, g_recv, f_send,
    p_send, p_recv, i_send, i_recv, o_sem, x_send, x_recv, y_send, y_recv, load_sem,
):
    half = lax.axis_index("tm")
    me = lax.axis_index("stn")
    chan = lax.axis_index("chan")
    row, col = me // RING, me % RING
    up = row * RING + lax.rem(col + 1, RING)
    down = row * RING + lax.rem(col + 3, RING)
    far = row * RING + lax.rem(col + 2, RING)
    pair = (1 - row) * RING + col
    peers = {0: me, 1: up, 2: far, 3: down, 4: pair}

    def remote(src, dst, send, recv, **where):
        return pltpu.make_async_remote_copy(
            src_ref=src, dst_ref=dst, send_sem=send, recv_sem=recv,
            device_id=where, device_id_type=MESH,
        )

    barrier = pltpu.get_barrier_semaphore()
    pl.semaphore_signal(barrier, inc=1, device_id={"tm": 1 - half}, device_id_type=MESH)
    for step in range(1, STN):
        pl.semaphore_signal(
            barrier, inc=1, device_id={"stn": lax.rem(me + step, STN)}, device_id_type=MESH
        )
    for step in range(1, CHAN):
        pl.semaphore_signal(
            barrier, inc=1, device_id={"chan": lax.rem(chan + step, CHAN)}, device_id_type=MESH
        )

    loads = [
        pltpu.make_async_copy(source, target, load_sem.at[k])
        for k, (source, target) in enumerate(
            (
                (map_hbm, map_ref), (row_hbm, row_ref), (table_hbm, table_ref),
                (v_hbm, v_ref), (taps_hbm, taps_ref), (tab_hbm, tab_ref),
            )
        )
    ]
    for load in loads:
        load.start()
    loads[0].wait()
    loads[1].wait()

    dishes = STN * SHARE
    line_id = lax.broadcasted_iota(jnp.int32, (dishes, dishes), 0)
    column_id = lax.broadcasted_iota(jnp.int32, (dishes, dishes), 1)

    def over_lanes(mask, value):
        return jnp.sum(jnp.where(mask, value, 0).astype(F32), axis=1, keepdims=True)

    def over_lines(mask, value):
        return jnp.sum(jnp.where(mask, value, 0).astype(F32), axis=0, keepdims=True)

    station_all = jnp.broadcast_to(map_ref[...], (dishes, dishes))
    row_all = jnp.broadcast_to(row_ref[...], (dishes, dishes))
    holder_across = station_all // OWN
    holder_line = over_lanes(line_id == column_id, holder_across).astype(jnp.int32)
    holder_down = jnp.broadcast_to(holder_line, (dishes, dishes))
    same = holder_across == holder_down
    rank_across = over_lines(same & (line_id < column_id), 1).astype(jnp.int32)
    hot = holder_across * SHARE + rank_across == line_id
    station_slot = over_lanes(hot, station_all % OWN).astype(jnp.int32)
    row_slot = over_lanes(hot, row_all).astype(jnp.int32)

    loads[2].wait()
    rows = table_ref.shape[2]
    weight_re, weight_im = table_ref[0].astype(F32), table_ref[1].astype(F32)
    blank = jnp.zeros((LANES - 2 * OWN * BEAMS, rows), F32)
    row_hot = (row_slot == lax.broadcasted_iota(jnp.int32, (dishes, rows), 1)).astype(F32)
    lane_station = lax.broadcasted_iota(jnp.int32, (dishes, LANES), 1) // BEAMS % OWN
    chosen = []
    for first, second in ((weight_re, weight_im), (-weight_im, weight_re)):
        spread = jnp.concatenate([first] * OWN + [second] * OWN + [blank], axis=0)
        value = lax.dot_general(
            row_hot.astype(BF16), spread.astype(BF16), (((1,), (1,)), ((), ())),
            preferred_element_type=F32,
        )
        chosen.append(jnp.where(lane_station == station_slot, value, 0.0))
    for holder in range(STN):
        lines = slice(holder * SHARE, (holder + 1) * SHARE)
        wt_ref[holder] = jnp.concatenate([part[lines] for part in chosen], axis=0).astype(BF16)
    loads[3].wait()

    def regrouped(holder, store):
        for part in range(2):
            for e in range(SHARE):
                dish = perm_ref[holder * SHARE + e]
                line = (part * SHARE + e) * PITCH
                regroup[line : line + FRAMES * NT * POL, :] = v_ref[part, dish].astype(F32)
        for pol in range(POL):
            for tile in range(FRAMES * NT):
                value = regroup[pl.ds(tile * POL + pol, 2 * SHARE, stride=PITCH), :]
                store(pol, tile * LANES, value.astype(BF16))

    mine = pl.ds(pl.multiple_of(me * 2 * SHARE, 2 * SHARE), 2 * SHARE)

    def holder_at(step):
        rows_away, ring_away = ROUTE[step]
        return (1 - row if rows_away else row) * RING + lax.rem(col + ring_away, RING)

    def dish_copy(pol, step):
        return remote(
            send_v.at[step, pol], recv_v.at[pol, mine],
            a_send.at[pol, step], a_recv.at[pol, step], stn=holder_at(step),
        )

    def weight_copy(step):
        holder = holder_at(step)
        return remote(
            wt_ref.at[holder], recv_wt.at[mine], w_send.at[step], w_recv.at[step], stn=holder
        )

    def prepare(step):
        def store(pol, lane, value):
            send_v[step, pol, :, lane : lane + LANES] = value

        regrouped(holder_at(step), store)

    steps = range(STN - 1)
    prepare(0)
    prepare(1)
    pl.semaphore_wait(barrier, 1 + (STN - 1) + (CHAN - 1))
    for step in steps:
        if step >= 2:
            prepare(step)
        if step >= 1:
            dish_copy(0, step - 1).start()

    def store_own(pol, lane, value):
        recv_v[pol, mine, lane : lane + LANES] = value

    regrouped(me, store_own)
    dish_copy(0, STN - 2).start()
    for step in steps:
        weight_copy(step).start()
        dish_copy(1, step).start()
    recv_wt[mine, :] = wt_ref[me]
    power[...] = jnp.zeros_like(power)
    lane_id = lax.broadcasted_iota(jnp.int32, (BEAMS, LANES), 1)

    for step in steps:
        weight_copy(step).wait_recv()
    weights[...] = jnp.transpose(recv_wt[...].astype(F32))[: 2 * OWN * BEAMS, :].astype(BF16)

    def halo_copy(pol):
        return remote(
            beams.at[pol, :, pl.ds((HISTORY + 1) * BEAMS, HISTORY * BEAMS), :],
            beams.at[pol, :, pl.ds(0, HISTORY * BEAMS), :],
            h_send.at[pol], h_recv.at[pol], tm=1 - half,
        )

    def chunk_copy(chunk, way):
        slot, target = ((3, up), (1, down), (4, pair))[way]
        return remote(
            formed.at[0, chunk], formed.at[slot, chunk],
            g_send.at[way, chunk], g_recv.at[slot, chunk], stn=target,
        )

    loads[4].wait()
    loads[5].wait()
    UP, DOWN, PAIR = range(3)

    def send_first(station, carry):
        chunk_copy(station, UP).start()
        chunk_copy(lax.rem(station + HALF, OWN), DOWN).start()
        chunk_copy(station, PAIR).start()
        return carry

    for pol in range(POL):
        for step in steps:
            dish_copy(pol, step).wait_recv()

        def steer(frame, carry):
            lanes = pl.ds(pl.multiple_of(frame * FINE, FINE), FINE)
            value = jnp.dot(weights[...], recv_v[pol, :, lanes], preferred_element_type=F32)
            line = pl.ds(pl.multiple_of((HISTORY + frame) * BEAMS, BEAMS), BEAMS)
            for j in range(2 * OWN):
                beams[pol, j, line, :] = value[j * BEAMS : (j + 1) * BEAMS, :]
            return carry

        lax.fori_loop(0, FRAMES, steer, 0)

        @pl.when(half == 0)
        def _():
            beams[pol, :, : HISTORY * BEAMS, :] = jnp.zeros((2 * OWN, HISTORY * BEAMS, FINE), F32)
            halo_copy(pol).start()

        @pl.when(half == 1)
        def _():
            halo_copy(pol).wait_recv()

        def filter_station(station, carry):
            for part in range(2):
                for tile in range(NT):
                    lanes = slice(tile * LANES, (tile + 1) * LANES)
                    taps = [
                        jnp.broadcast_to(taps_ref[j : j + 1, lanes], (BEAMS, LANES))
                        for j in range(TAPS)
                    ]
                    outs = []
                    for frame in range(FRAMES):
                        total = None
                        for j in range(TAPS):
                            line = (frame + HISTORY - j) * BEAMS
                            term = taps[j] * beams[
                                pol, part * OWN + station, line : line + BEAMS, lanes
                            ]
                            total = term if total is None else total + term
                        outs.append(total)
                        if frame % 2:
                            base = pl.multiple_of(
                                station * FRAMES * BEAMS + (frame - 1) * BEAMS, 2 * BEAMS
                            )
                            lane = part * FINE + tile * LANES
                            filtered[pl.ds(base, 2 * BEAMS), lane : lane + LANES] = (
                                jnp.concatenate(outs, axis=0).astype(BF16)
                            )
                            outs = []
            return carry

        lax.fori_loop(0, OWN, filter_station, 0)

        def transform(station, carry):
            lines = pl.ds(pl.multiple_of(station * FRAMES * BEAMS, FRAMES * BEAMS), FRAMES * BEAMS)
            value = jnp.dot(filtered[lines, :], tab_ref[...], preferred_element_type=F32)
            formed[0, pol * OWN + station] = value.astype(BF16)
            squares = jnp.sum((value * value).reshape(FRAMES, BEAMS, 2 * FINE), axis=0)
            squares = sum(squares[:, k * LANES : (k + 1) * LANES] for k in range(4))
            total = jnp.sum(squares, axis=1, keepdims=True)
            power[...] += jnp.where(lane_id == station * POL + pol, total, 0.0)
            return carry

        lax.fori_loop(0, OWN, transform, 0)

        if pol == 0:
            lax.fori_loop(0, OWN, send_first, 0)

    def arrived(slot, chunk):
        remote(
            formed.at[slot, chunk], formed.at[slot, chunk], g_send.at[0, chunk],
            g_recv.at[slot, chunk], stn=up,
        ).wait_recv()

    def forward_up(pol, n):
        chunk = pol * OWN + n
        return remote(
            formed.at[3, chunk], formed.at[2, chunk],
            f_send.at[0, pol, n], g_recv.at[2, chunk], stn=up,
        )

    def forward_down(pol, n):
        chunk = pol * OWN + HALF + n
        return remote(
            formed.at[1, chunk], formed.at[2, chunk],
            f_send.at[1, pol, n], g_recv.at[2, chunk], stn=down,
        )

    def power_copy(step):
        return remote(
            power, power_all.at[step - 1], p_send.at[step - 1], p_recv.at[step - 1],
            chan=lax.rem(chan + step, CHAN),
        )

    for step in range(1, CHAN):
        power_copy(step).start()

    def send_second(n, carry):
        chunk_copy(OWN + n, UP).start()
        chunk_copy(OWN + HALF + n, DOWN).start()
        chunk_copy(OWN + 2 * n, PAIR).start()
        chunk_copy(OWN + 2 * n + 1, PAIR).start()
        arrived(3, n)
        forward_up(0, n).start()
        arrived(1, HALF + n)
        forward_down(0, n).start()
        return carry

    lax.fori_loop(0, HALF, send_second, 0)
    for step in range(1, CHAN):
        power_copy(step).wait_recv()
    total = power[...]
    for step in range(1, CHAN):
        total = total + power_all[step - 1]
    inverse[0] = lax.rsqrt(total / DENOMINATOR + EPSILON)
    inverse_copies = [
        remote(inverse.at[0], inverse.at[slot], i_send.at[slot], i_recv.at[slot], stn=target)
        for slot, target in ((1, down), (2, far), (3, up), (4, pair))
    ]

    def lane_of(slot, index):
        tile = inverse[slot]
        one = jnp.sum(jnp.where(lane_id == index, tile, 0.0), axis=1, keepdims=True)
        return jnp.broadcast_to(one, (BEAMS, LANES))

    def scale_chunk(which, slot, station):
        for pol in range(POL):
            factor = lane_of(slot, station * POL + pol) * (1.0 / FRAMES)
            for pairs in range(FRAMES // 2):
                lines = slice(pairs * 2 * BEAMS, (pairs + 1) * 2 * BEAMS)
                for tile in range(4):
                    lanes = slice(tile * LANES, (tile + 1) * LANES)
                    value = formed[slot, pol * OWN + station, lines, lanes].astype(F32)
                    scaled[which, station * POL + pol, lines, lanes] = jnp.concatenate(
                        [value[:BEAMS] * factor, value[BEAMS:] * factor], axis=0
                    )

    def correlate(which, slot, station, swapped):
        for q in range(POL):
            factor = lane_of(slot, station * POL + q)
            for tile in range(NT):
                re_lanes = slice(tile * LANES, (tile + 1) * LANES)
                im_lanes = slice(FINE + tile * LANES, FINE + (tile + 1) * LANES)
                real = [None] * (OWN * POL)
                imag = [None] * (OWN * POL)
                for pairs in range(FRAMES // 2):
                    lines = slice(pairs * 2 * BEAMS, (pairs + 1) * 2 * BEAMS)
                    right_re = formed[slot, q * OWN + station, lines, re_lanes].astype(F32)
                    right_im = formed[slot, q * OWN + station, lines, im_lanes].astype(F32)
                    for part in range(2):
                        cr = right_re[part * BEAMS : (part + 1) * BEAMS]
                        ci = right_im[part * BEAMS : (part + 1) * BEAMS]
                        line = (pairs * 2 + part) * BEAMS
                        for c in range(OWN * POL):
                            ar = scaled[which, c, line : line + BEAMS, re_lanes]
                            ai = scaled[which, c, line : line + BEAMS, im_lanes]
                            re = ar * cr + ai * ci
                            im = ar * ci - ai * cr if swapped else ai * cr - ar * ci
                            real[c] = re if real[c] is None else real[c] + re
                            imag[c] = im if imag[c] is None else imag[c] + im
                for c in range(OWN * POL):
                    s, p = c // POL, c % POL
                    line = q * 4 + tile * 2 + p if swapped else p * 4 + tile * 2 + q
                    lines = pl.ds(line, BEAMS, stride=8)
                    stage[0, s, lines, :] = real[c] * factor
                    stage[1, s, lines, :] = imag[c] * factor

    def out_copy(unit, block, station):
        return pltpu.make_async_copy(
            packed.at[unit], out_ref.at[:, :, block * OWN + station], o_sem.at[unit]
        )

    for copy in inverse_copies:
        copy.start()

    def own_scale(station, carry):
        scale_chunk(0, 0, station)
        return carry

    lax.fori_loop(0, OWN, own_scale, 0)

    def own_pairs(station, carry):
        correlate(0, 0, station, False)
        packed[station] = stage[...].astype(BF16)
        out_copy(station, me, station).start()
        return carry

    lax.fori_loop(0, OWN, own_pairs, 0)
    for copy in inverse_copies:
        copy.wait_recv()

    def neighbour_pairs(n, station):
        slot = 3 - 2 * n
        unit = slot * OWN + station
        correlate(0, slot, station, False)
        packed[unit] = stage[...].astype(BF16)
        out_copy(unit, row * RING + lax.rem(col + slot, RING), station).start()

    def first_pairs(k, carry):
        arrived(3, OWN + k)
        forward_up(1, k).start()
        arrived(1, OWN + HALF + k)
        forward_down(1, k).start()
        chunk_copy(OWN + HALF + k, UP).start()
        chunk_copy(OWN + k, DOWN).start()

        def near(n, c):
            neighbour_pairs(n, k + HALF * n)
            return c

        lax.fori_loop(0, 2, near, 0)

        def partner(n, c):
            station = 2 * k + n
            arrived(4, station)
            arrived(4, OWN + station)
            scale_chunk(1, 4, station)
            unit = 4 * OWN + station
            correlate(0, 4, station, False)
            packed[unit] = stage[...].astype(BF16)
            out_copy(unit, pair, station).start()
            return c

        lax.fori_loop(0, 2, partner, 0)
        return carry

    lax.fori_loop(0, HALF, first_pairs, 0)

    across = [(1 - row) * RING + lax.rem(col + step, RING) for step in range(RING)]

    def swap_copy(n, station):
        return remote(
            packed.at[5 * OWN + n * OWN + station], land_swap.at[n, station],
            x_send.at[n, station], x_recv.at[n, station],
            stn=row * RING + lax.rem(col + 3 - 2 * n, RING),
        )

    def far_copy(station):
        return remote(
            packed.at[7 * OWN + station], land_far.at[station],
            y_send.at[station], y_recv.at[station], stn=pair,
        )

    def swap_out(n, station):
        block = (1 - row) * RING + lax.rem(col + 1 + 2 * n, RING)
        stations = pl.ds(pl.multiple_of(block * OWN, OWN), OWN)
        return pltpu.make_async_copy(
            land_swap.at[n, station], out_ref.at[:, station, stations], x_recv.at[n, station]
        )

    def far_out(station):
        return pltpu.make_async_copy(
            land_far.at[station], out_ref.at[:, :, across[2] * OWN + station], y_recv.at[station]
        )

    def swapped_pairs(n, station):
        correlate(1, 3 - 2 * n, station, True)
        packed[5 * OWN + n * OWN + station] = stage[...].astype(BF16)
        swap_copy(n, station).start()

    def first_swaps(k, carry):
        n = lax.rem(k, 2)
        swapped_pairs(n, k // 2 + HALF * n)
        return carry

    def far_pairs(k, carry):
        station = lax.rem(k, 2) * HALF + k // 2
        arrived(2, station)
        arrived(2, OWN + station)
        correlate(1, 2, station, False)
        packed[7 * OWN + station] = stage[...].astype(BF16)
        far_copy(station).start()
        return carry

    def last_pairs(k, carry):
        n = lax.rem(k, 2)
        station = lax.rem(HALF + k // 2 + HALF * n, OWN)
        slot = 3 - 2 * n
        arrived(slot, station)
        arrived(slot, OWN + station)
        swapped_pairs(n, station)
        neighbour_pairs(n, station)
        return carry

    def far_own_pairs(station, carry):
        unit = 2 * OWN + station
        correlate(0, 2, station, False)
        packed[unit] = stage[...].astype(BF16)
        out_copy(unit, far, station).start()
        return carry

    lax.fori_loop(0, 2 * HALF, first_swaps, 0)
    lax.fori_loop(0, OWN, far_pairs, 0)
    lax.fori_loop(0, 2 * HALF, last_pairs, 0)
    lax.fori_loop(0, OWN, far_own_pairs, 0)

    def land_far_pairs(station, carry):
        far_copy(station).wait_recv()
        far_out(station).start()
        return carry

    def land_swaps(k, carry):
        n = lax.rem(k, 2)
        station = lax.rem(k // 2 + HALF * n, OWN)
        swap_copy(n, station).wait_recv()
        swap_out(n, station).start()
        return carry

    lax.fori_loop(0, OWN, land_far_pairs, 0)
    lax.fori_loop(0, 2 * OWN, land_swaps, 0)

    def finish(station, carry):
        for n in range(2):
            swap_copy(n, station).wait_send()
            swap_out(n, station).wait()
        far_copy(station).wait_send()
        far_out(station).wait()
        for slot in range(5):
            out_copy(slot * OWN + station, peers[slot], station).wait()
        for pol in range(POL):
            for way in (UP, DOWN, PAIR):
                chunk_copy(pol * OWN + station, way).wait_send()
        return carry

    lax.fori_loop(0, OWN, finish, 0)
    for pol in range(POL):
        for n in range(HALF):
            forward_up(pol, n).wait_send()
            forward_down(pol, n).wait_send()
    for step in steps:
        dish_copy(0, step).wait_send()
        dish_copy(1, step).wait_send()
        weight_copy(step).wait_send()
    for step in range(1, CHAN):
        power_copy(step).wait_send()
    for copy in inverse_copies:
        copy.wait_send()

    @pl.when(half == 0)
    def _():
        for pol in range(POL):
            halo_copy(pol).wait_send()


def widen(narrow_hbm, wide_hbm, narrow, wide, in_sem, out_sem):
    size = narrow.shape[0] // WIDEN_STEPS
    pieces = [pl.ds(step * size, size) for step in range(WIDEN_STEPS)]
    loads = [
        pltpu.make_async_copy(narrow_hbm.at[piece], narrow.at[piece], in_sem.at[step])
        for step, piece in enumerate(pieces)
    ]
    stores = [
        pltpu.make_async_copy(wide.at[piece], wide_hbm.at[piece], out_sem.at[step])
        for step, piece in enumerate(pieces)
    ]
    for load in loads:
        load.start()
    for piece, load, store in zip(pieces, loads, stores):
        load.wait()
        wide[piece] = narrow[piece].astype(F32)
        store.start()
    for store in stores:
        store.wait()


def widened(array):
    shape = array.shape
    flat = array.reshape(-1, LANES)
    hbm = pl.BlockSpec(memory_space=pltpu.HBM)
    wide = pl.pallas_call(
        widen,
        out_shape=jax.ShapeDtypeStruct(flat.shape, F32),
        in_specs=[hbm],
        out_specs=hbm,
        scratch_shapes=[
            pltpu.VMEM(flat.shape, BF16), pltpu.VMEM(flat.shape, F32),
            pltpu.SemaphoreType.DMA((WIDEN_STEPS,)), pltpu.SemaphoreType.DMA((WIDEN_STEPS,)),
        ],
        compiler_params=pltpu.CompilerParams(vmem_limit_bytes=WIDEN_GRANT),
    )(flat)
    return wide.reshape(shape)


def dish_order(station_map):
    index = jnp.arange(station_map.shape[0], dtype=jnp.int32)
    holder = station_map // OWN
    earlier = (holder[:, None] == holder[None, :]) & (index[None, :] < index[:, None])
    slot = holder * SHARE + jnp.sum(earlier.astype(jnp.int32), axis=1)
    return jnp.sum(jnp.where(slot[None, :] == index[:, None], index[None, :], 0), axis=1)


def per_device(voltages, fir_taps, station_map, beam_index, weight_table):
    parts, _, dishes, frames, pols, fine = voltages.shape
    rows = voltages.reshape(parts, dishes, frames, pols, NT, LANES)
    rows = rows.swapaxes(3, 4).reshape(parts, dishes, frames * NT * pols, LANES)
    table = jnp.asarray(dft_table(), BF16)
    weights = jnp.transpose(weight_table[:, :, 0, :], (0, 2, 1))
    hbm = pl.BlockSpec(memory_space=pltpu.HBM)
    dma = pltpu.SemaphoreType.DMA
    chunk = (FRAMES * BEAMS, 2 * FINE)
    operands = (
        station_map[None], beam_index[None], weights, rows, fir_taps, table,
    )
    result = pl.pallas_call(
        kernel,
        out_shape=jax.ShapeDtypeStruct((2, OWN, STN * OWN, 8 * BEAMS, LANES), BF16),
        in_specs=[pl.BlockSpec(memory_space=pltpu.SMEM)] + [hbm] * len(operands),
        out_specs=hbm,
        scratch_shapes=[
            *(pltpu.VMEM(a.shape, a.dtype) for a in operands),
            pltpu.VMEM((STN, 2 * SHARE, LANES), BF16),
            pltpu.VMEM((2 * SHARE * PITCH, LANES), F32),
            pltpu.VMEM((STN - 1, POL, 2 * SHARE, FRAMES * FINE), BF16),
            pltpu.VMEM((POL, STN * 2 * SHARE, FRAMES * FINE), BF16),
            pltpu.VMEM((STN * 2 * SHARE, LANES), BF16),
            pltpu.VMEM((2 * OWN * BEAMS, STN * 2 * SHARE), BF16),
            pltpu.VMEM((POL, 2 * OWN, (HISTORY + FRAMES) * BEAMS, FINE), F32),
            pltpu.VMEM((OWN * FRAMES * BEAMS, 2 * FINE), BF16),
            pltpu.VMEM((5, POL * OWN, *chunk), BF16),
            pltpu.VMEM((2, OWN * POL, *chunk), F32),
            pltpu.VMEM((2, OWN, 8 * BEAMS, LANES), F32),
            pltpu.VMEM((8 * OWN, 2, OWN, 8 * BEAMS, LANES), BF16),
            pltpu.VMEM((2, OWN, 2, OWN, 8 * BEAMS, LANES), BF16),
            pltpu.VMEM((OWN, 2, OWN, 8 * BEAMS, LANES), BF16),
            pltpu.VMEM((BEAMS, LANES), F32),
            pltpu.VMEM((CHAN - 1, BEAMS, LANES), F32),
            pltpu.VMEM((5, BEAMS, LANES), F32),
            dma((POL, STN - 1)), dma((POL, STN - 1)),
            dma((STN - 1,)), dma((STN - 1,)),
            dma((POL,)), dma((POL,)),
            dma((3, POL * OWN)), dma((5, POL * OWN)), dma((2, POL, HALF)),
            dma((CHAN - 1,)), dma((CHAN - 1,)),
            dma((5,)), dma((5,)),
            dma((5 * OWN,)),
            dma((2, OWN)), dma((2, OWN)),
            dma((OWN,)), dma((OWN,)),
            dma((len(operands),)),
        ],
        compiler_params=pltpu.CompilerParams(
            collective_id=0, has_side_effects=True, vmem_limit_bytes=VMEM_GRANT
        ),
    )(dish_order(station_map), *operands)
    result = widened(result).reshape(2, OWN, STN * OWN, BEAMS, POL, NT, POL, LANES)
    result = result.swapaxes(5, 6).reshape(2, 1, OWN, STN * OWN, BEAMS, POL, POL, fine)
    return result[None]


def solution(mesh):
    in_specs = (
        P(None, "chan", "stn", "tm", None, None),
        P(),
        P("stn"),
        P("stn"),
        P(None, None, "chan", None),
    )
    out_specs = P("tm", None, "chan", "stn", None, None, None, None, None)
    return jax.shard_map(
        per_device, mesh=mesh, in_specs=in_specs, out_specs=out_specs, check_vma=False
    )
```

```python
import functools

import jax
import jax.numpy as jnp
import numpy as np
from jax import lax
from jax.experimental import pallas as pl
from jax.experimental.pallas import tpu as pltpu
from jax.sharding import PartitionSpec as P

MESH = pl.DeviceIdType.MESH
F32 = jnp.float32
BF16 = jnp.bfloat16
EPSILON = 1e-06
STN = 8
RING = 4
CHAN = 8
SHARE = 8
OWN = 4
HALF = OWN // 2
BEAMS = 8
POL = 2
FRAMES = 16
TAPS = 16
FINE = 256
LANES = 128
NT = FINE // LANES
HISTORY = TAPS - 1
VMEM_GRANT = 67043328 - 4 * 1024 * 1024
PITCH = 72
DENOMINATOR = float(CHAN * FRAMES * FINE)


WIDEN_STEPS = 16
WIDEN_GRANT = 62 * 1024 * 1024
ROUTE = ((1, 2), (1, 1), (1, 3), (1, 0), (0, 2), (0, 1), (0, 3))


def dft_table():
    step = np.arange(FINE)
    angle = (step[:, None] * step[None, :] % FINE) * (2.0 * np.pi / FINE)
    cosine, sine = np.cos(angle), np.sin(angle)
    return np.block([[cosine, -sine], [sine, cosine]]).astype(np.float32)


def kernel(
    map_hbm, row_hbm, table_hbm, v_hbm, taps_hbm, tab_hbm, out_ref,
    map_ref, row_ref, table_ref, v_ref, taps_ref, tab_ref, perm_vec, perm_ref, wt_ref, regroup, send_v, recv_v, recv_wt, weights, beams, filtered, formed, scaled, stage, packed, land_swap, land_far,
    power, power_all, inverse,
    a_send, a_recv, w_send, w_recv, h_send, h_recv, g_send, g_recv, f_send,
    p_send, p_recv, i_send, i_recv, o_sem, x_send, x_recv, y_send, y_recv, load_sem, perm_sem,
):
    half = lax.axis_index("tm")
    me = lax.axis_index("stn")
    chan = lax.axis_index("chan")
    row, col = me // RING, me % RING
    up = row * RING + lax.rem(col + 1, RING)
    down = row * RING + lax.rem(col + 3, RING)
    far = row * RING + lax.rem(col + 2, RING)
    pair = (1 - row) * RING + col
    peers = {0: me, 1: up, 2: far, 3: down, 4: pair}

    def remote(src, dst, send, recv, **where):
        return pltpu.make_async_remote_copy(
            src_ref=src, dst_ref=dst, send_sem=send, recv_sem=recv,
            device_id=where, device_id_type=MESH,
        )

    barrier = pltpu.get_barrier_semaphore()
    pl.semaphore_signal(barrier, inc=1, device_id={"tm": 1 - half}, device_id_type=MESH)
    for step in range(1, STN):
        pl.semaphore_signal(
            barrier, inc=1, device_id={"stn": lax.rem(me + step, STN)}, device_id_type=MESH
        )
    for step in range(1, CHAN):
        pl.semaphore_signal(
            barrier, inc=1, device_id={"chan": lax.rem(chan + step, CHAN)}, device_id_type=MESH
        )

    loads = [
        pltpu.make_async_copy(source, target, load_sem.at[k])
        for k, (source, target) in enumerate(
            (
                (map_hbm, map_ref), (row_hbm, row_ref), (table_hbm, table_ref),
                (v_hbm, v_ref), (taps_hbm, taps_ref), (tab_hbm, tab_ref),
            )
        )
    ]
    for load in loads:
        load.start()
    loads[0].wait()
    loads[1].wait()

    dishes = STN * SHARE
    line_id = lax.broadcasted_iota(jnp.int32, (dishes, dishes), 0)
    column_id = lax.broadcasted_iota(jnp.int32, (dishes, dishes), 1)

    def over_lanes(mask, value):
        return jnp.sum(jnp.where(mask, value, 0), axis=1, keepdims=True, dtype=jnp.int32)

    def over_lines(mask, value):
        return jnp.sum(jnp.where(mask, value, 0), axis=0, keepdims=True, dtype=jnp.int32)

    station_all = jnp.broadcast_to(map_ref[...], (dishes, dishes))
    row_all = jnp.broadcast_to(row_ref[...], (dishes, dishes))
    holder_across = station_all // OWN
    holder_line = over_lanes(line_id == column_id, holder_across)
    holder_down = jnp.broadcast_to(holder_line, (dishes, dishes))
    same = holder_across == holder_down
    rank_down = over_lanes(same & (column_id < line_id), 1)
    slot_down = holder_down * SHARE + rank_down
    perm_vec[...] = over_lines(slot_down == column_id, line_id)
    perm_copy = pltpu.make_async_copy(perm_vec, perm_ref, perm_sem)
    perm_copy.start()
    rank_across = over_lines(same & (line_id < column_id), 1)
    hot = holder_across * SHARE + rank_across == line_id
    station_slot = over_lanes(hot, station_all % OWN)
    row_slot = over_lanes(hot, row_all)

    loads[2].wait()
    rows = table_ref.shape[2]
    weight_re, weight_im = table_ref[0].astype(F32), table_ref[1].astype(F32)
    blank = jnp.zeros((LANES - 2 * OWN * BEAMS, rows), F32)
    row_hot = (row_slot == lax.broadcasted_iota(jnp.int32, (dishes, rows), 1)).astype(F32)
    lane_station = lax.broadcasted_iota(jnp.int32, (dishes, LANES), 1) // BEAMS % OWN
    chosen = []
    for first, second in ((weight_re, weight_im), (-weight_im, weight_re)):
        spread = jnp.concatenate([first] * OWN + [second] * OWN + [blank], axis=0)
        value = lax.dot_general(
            row_hot.astype(BF16), spread.astype(BF16), (((1,), (1,)), ((), ())),
            preferred_element_type=F32,
        )
        chosen.append(jnp.where(lane_station == station_slot, value, 0.0))
    for holder in range(STN):
        lines = slice(holder * SHARE, (holder + 1) * SHARE)
        wt_ref[holder] = jnp.concatenate([part[lines] for part in chosen], axis=0).astype(BF16)
    loads[3].wait()
    perm_copy.wait()

    def regrouped(holder, store):
        for part in range(2):
            for e in range(SHARE):
                dish = perm_ref[0, holder * SHARE + e]
                line = (part * SHARE + e) * PITCH
                regroup[line : line + FRAMES * NT * POL, :] = v_ref[part, dish].astype(F32)
        for pol in range(POL):
            for tile in range(FRAMES * NT):
                value = regroup[pl.ds(tile * POL + pol, 2 * SHARE, stride=PITCH), :]
                store(pol, tile * LANES, value.astype(BF16))

    mine = pl.ds(pl.multiple_of(me * 2 * SHARE, 2 * SHARE), 2 * SHARE)

    def holder_at(step):
        rows_away, ring_away = ROUTE[step]
        return (1 - row if rows_away else row) * RING + lax.rem(col + ring_away, RING)

    def dish_copy(pol, step):
        return remote(
            send_v.at[step, pol], recv_v.at[pol, mine],
            a_send.at[pol, step], a_recv.at[pol, step], stn=holder_at(step),
        )

    def weight_copy(step):
        holder = holder_at(step)
        return remote(
            wt_ref.at[holder], recv_wt.at[mine], w_send.at[step], w_recv.at[step], stn=holder
        )

    def prepare(step):
        def store(pol, lane, value):
            send_v[step, pol, :, lane : lane + LANES] = value

        regrouped(holder_at(step), store)

    steps = range(STN - 1)
    prepare(0)
    prepare(1)
    pl.semaphore_wait(barrier, 1 + (STN - 1) + (CHAN - 1))
    for step in steps:
        if step >= 2:
            prepare(step)
        if step >= 1:
            dish_copy(0, step - 1).start()

    def store_own(pol, lane, value):
        recv_v[pol, mine, lane : lane + LANES] = value

    regrouped(me, store_own)
    dish_copy(0, STN - 2).start()
    for step in steps:
        weight_copy(step).start()
        dish_copy(1, step).start()
    recv_wt[mine, :] = wt_ref[me]
    power[...] = jnp.zeros_like(power)
    lane_id = lax.broadcasted_iota(jnp.int32, (BEAMS, LANES), 1)

    for step in steps:
        weight_copy(step).wait_recv()
    weights[...] = jnp.transpose(recv_wt[...].astype(F32))[: 2 * OWN * BEAMS, :].astype(BF16)

    def halo_copy(pol):
        return remote(
            beams.at[pol, :, pl.ds((HISTORY + 1) * BEAMS, HISTORY * BEAMS), :],
            beams.at[pol, :, pl.ds(0, HISTORY * BEAMS), :],
            h_send.at[pol], h_recv.at[pol], tm=1 - half,
        )

    def chunk_copy(chunk, way):
        slot, target = ((3, up), (1, down), (4, pair))[way]
        return remote(
            formed.at[0, chunk], formed.at[slot, chunk],
            g_send.at[way, chunk], g_recv.at[slot, chunk], stn=target,
        )

    loads[4].wait()
    loads[5].wait()
    UP, DOWN, PAIR = range(3)

    def send_first(station, carry):
        chunk_copy(station, UP).start()
        chunk_copy(lax.rem(station + HALF, OWN), DOWN).start()
        chunk_copy(station, PAIR).start()
        return carry

    for pol in range(POL):
        for step in steps:
            dish_copy(pol, step).wait_recv()

        def steer(frame, carry):
            lanes = pl.ds(pl.multiple_of(frame * FINE, FINE), FINE)
            value = jnp.dot(weights[...], recv_v[pol, :, lanes], preferred_element_type=F32)
            line = pl.ds(pl.multiple_of((HISTORY + frame) * BEAMS, BEAMS), BEAMS)
            for j in range(2 * OWN):
                beams[pol, j, line, :] = value[j * BEAMS : (j + 1) * BEAMS, :]
            return carry

        lax.fori_loop(0, FRAMES, steer, 0)

        @pl.when(half == 0)
        def _():
            beams[pol, :, : HISTORY * BEAMS, :] = jnp.zeros((2 * OWN, HISTORY * BEAMS, FINE), F32)
            halo_copy(pol).start()

        @pl.when(half == 1)
        def _():
            halo_copy(pol).wait_recv()

        def filter_station(station, carry):
            for part in range(2):
                for tile in range(NT):
                    lanes = slice(tile * LANES, (tile + 1) * LANES)
                    taps = [
                        jnp.broadcast_to(taps_ref[j : j + 1, lanes], (BEAMS, LANES))
                        for j in range(TAPS)
                    ]
                    outs = []
                    for frame in range(FRAMES):
                        total = None
                        for j in range(TAPS):
                            line = (frame + HISTORY - j) * BEAMS
                            term = taps[j] * beams[
                                pol, part * OWN + station, line : line + BEAMS, lanes
                            ]
                            total = term if total is None else total + term
                        outs.append(total)
                        if frame % 2:
                            base = pl.multiple_of(
                                station * FRAMES * BEAMS + (frame - 1) * BEAMS, 2 * BEAMS
                            )
                            lane = part * FINE + tile * LANES
                            filtered[pl.ds(base, 2 * BEAMS), lane : lane + LANES] = (
                                jnp.concatenate(outs, axis=0).astype(BF16)
                            )
                            outs = []
            return carry

        lax.fori_loop(0, OWN, filter_station, 0)

        def transform(station, carry):
            lines = pl.ds(pl.multiple_of(station * FRAMES * BEAMS, FRAMES * BEAMS), FRAMES * BEAMS)
            value = jnp.dot(filtered[lines, :], tab_ref[...], preferred_element_type=F32)
            formed[0, pol * OWN + station] = value.astype(BF16)
            squares = jnp.sum((value * value).reshape(FRAMES, BEAMS, 2 * FINE), axis=0)
            squares = sum(squares[:, k * LANES : (k + 1) * LANES] for k in range(4))
            total = jnp.sum(squares, axis=1, keepdims=True)
            power[...] += jnp.where(lane_id == station * POL + pol, total, 0.0)
            return carry

        lax.fori_loop(0, OWN, transform, 0)

        if pol == 0:
            lax.fori_loop(0, OWN, send_first, 0)

    def arrived(slot, chunk):
        remote(
            formed.at[slot, chunk], formed.at[slot, chunk], g_send.at[0, chunk],
            g_recv.at[slot, chunk], stn=up,
        ).wait_recv()

    def forward_up(pol, n):
        chunk = pol * OWN + n
        return remote(
            formed.at[3, chunk], formed.at[2, chunk],
            f_send.at[0, pol, n], g_recv.at[2, chunk], stn=up,
        )

    def forward_down(pol, n):
        chunk = pol * OWN + HALF + n
        return remote(
            formed.at[1, chunk], formed.at[2, chunk],
            f_send.at[1, pol, n], g_recv.at[2, chunk], stn=down,
        )

    def power_copy(step):
        return remote(
            power, power_all.at[step - 1], p_send.at[step - 1], p_recv.at[step - 1],
            chan=lax.rem(chan + step, CHAN),
        )

    for step in range(1, CHAN):
        power_copy(step).start()

    def send_second(n, carry):
        chunk_copy(OWN + n, UP).start()
        chunk_copy(OWN + HALF + n, DOWN).start()
        chunk_copy(OWN + 2 * n, PAIR).start()
        chunk_copy(OWN + 2 * n + 1, PAIR).start()
        arrived(3, n)
        forward_up(0, n).start()
        arrived(1, HALF + n)
        forward_down(0, n).start()
        return carry

    lax.fori_loop(0, HALF, send_second, 0)
    for step in range(1, CHAN):
        power_copy(step).wait_recv()
    total = power[...]
    for step in range(1, CHAN):
        total = total + power_all[step - 1]
    inverse[0] = lax.rsqrt(total / DENOMINATOR + EPSILON)
    inverse_copies = [
        remote(inverse.at[0], inverse.at[slot], i_send.at[slot], i_recv.at[slot], stn=target)
        for slot, target in ((1, down), (2, far), (3, up), (4, pair))
    ]

    def lane_of(slot, index):
        tile = inverse[slot]
        one = jnp.sum(jnp.where(lane_id == index, tile, 0.0), axis=1, keepdims=True)
        return jnp.broadcast_to(one, (BEAMS, LANES))

    def scale_chunk(which, slot, station):
        for pol in range(POL):
            factor = lane_of(slot, station * POL + pol) * (1.0 / FRAMES)
            for pairs in range(FRAMES // 2):
                lines = slice(pairs * 2 * BEAMS, (pairs + 1) * 2 * BEAMS)
                for tile in range(4):
                    lanes = slice(tile * LANES, (tile + 1) * LANES)
                    value = formed[slot, pol * OWN + station, lines, lanes].astype(F32)
                    scaled[which, station * POL + pol, lines, lanes] = jnp.concatenate(
                        [value[:BEAMS] * factor, value[BEAMS:] * factor], axis=0
                    )

    def correlate(which, slot, station, swapped):
        for q in range(POL):
            factor = lane_of(slot, station * POL + q)
            for tile in range(NT):
                re_lanes = slice(tile * LANES, (tile + 1) * LANES)
                im_lanes = slice(FINE + tile * LANES, FINE + (tile + 1) * LANES)
                real = [None] * (OWN * POL)
                imag = [None] * (OWN * POL)
                for pairs in range(FRAMES // 2):
                    lines = slice(pairs * 2 * BEAMS, (pairs + 1) * 2 * BEAMS)
                    right_re = formed[slot, q * OWN + station, lines, re_lanes].astype(F32)
                    right_im = formed[slot, q * OWN + station, lines, im_lanes].astype(F32)
                    for part in range(2):
                        cr = right_re[part * BEAMS : (part + 1) * BEAMS]
                        ci = right_im[part * BEAMS : (part + 1) * BEAMS]
                        line = (pairs * 2 + part) * BEAMS
                        for c in range(OWN * POL):
                            ar = scaled[which, c, line : line + BEAMS, re_lanes]
                            ai = scaled[which, c, line : line + BEAMS, im_lanes]
                            re = ar * cr + ai * ci
                            im = ar * ci - ai * cr if swapped else ai * cr - ar * ci
                            real[c] = re if real[c] is None else real[c] + re
                            imag[c] = im if imag[c] is None else imag[c] + im
                for c in range(OWN * POL):
                    s, p = c // POL, c % POL
                    line = q * 4 + tile * 2 + p if swapped else p * 4 + tile * 2 + q
                    lines = pl.ds(line, BEAMS, stride=8)
                    stage[0, s, lines, :] = real[c] * factor
                    stage[1, s, lines, :] = imag[c] * factor

    def out_copy(unit, block, station):
        return pltpu.make_async_copy(
            packed.at[unit], out_ref.at[:, :, block * OWN + station], o_sem.at[unit]
        )

    for copy in inverse_copies:
        copy.start()

    def own_scale(station, carry):
        scale_chunk(0, 0, station)
        return carry

    lax.fori_loop(0, OWN, own_scale, 0)

    def own_pairs(station, carry):
        correlate(0, 0, station, False)
        packed[station] = stage[...].astype(BF16)
        out_copy(station, me, station).start()
        return carry

    lax.fori_loop(0, OWN, own_pairs, 0)
    for copy in inverse_copies:
        copy.wait_recv()

    def neighbour_pairs(n, station):
        slot = 3 - 2 * n
        unit = slot * OWN + station
        correlate(0, slot, station, False)
        packed[unit] = stage[...].astype(BF16)
        out_copy(unit, row * RING + lax.rem(col + slot, RING), station).start()

    def first_pairs(k, carry):
        arrived(3, OWN + k)
        forward_up(1, k).start()
        arrived(1, OWN + HALF + k)
        forward_down(1, k).start()
        chunk_copy(OWN + HALF + k, UP).start()
        chunk_copy(OWN + k, DOWN).start()

        def near(n, c):
            neighbour_pairs(n, k + HALF * n)
            return c

        lax.fori_loop(0, 2, near, 0)

        def partner(n, c):
            station = 2 * k + n
            arrived(4, station)
            arrived(4, OWN + station)
            scale_chunk(1, 4, station)
            unit = 4 * OWN + station
            correlate(0, 4, station, False)
            packed[unit] = stage[...].astype(BF16)
            out_copy(unit, pair, station).start()
            return c

        lax.fori_loop(0, 2, partner, 0)
        return carry

    lax.fori_loop(0, HALF, first_pairs, 0)

    across = [(1 - row) * RING + lax.rem(col + step, RING) for step in range(RING)]

    def swap_copy(n, station):
        return remote(
            packed.at[5 * OWN + n * OWN + station], land_swap.at[n, station],
            x_send.at[n, station], x_recv.at[n, station],
            stn=row * RING + lax.rem(col + 3 - 2 * n, RING),
        )

    def far_copy(station):
        return remote(
            packed.at[7 * OWN + station], land_far.at[station],
            y_send.at[station], y_recv.at[station], stn=pair,
        )

    def swap_out(n, station):
        block = (1 - row) * RING + lax.rem(col + 1 + 2 * n, RING)
        stations = pl.ds(pl.multiple_of(block * OWN, OWN), OWN)
        return pltpu.make_async_copy(
            land_swap.at[n, station], out_ref.at[:, station, stations], x_recv.at[n, station]
        )

    def far_out(station):
        return pltpu.make_async_copy(
            land_far.at[station], out_ref.at[:, :, across[2] * OWN + station], y_recv.at[station]
        )

    def swapped_pairs(n, station):
        correlate(1, 3 - 2 * n, station, True)
        packed[5 * OWN + n * OWN + station] = stage[...].astype(BF16)
        swap_copy(n, station).start()

    def first_swaps(k, carry):
        n = lax.rem(k, 2)
        swapped_pairs(n, k // 2 + HALF * n)
        return carry

    def far_pairs(k, carry):
        station = lax.rem(k, 2) * HALF + k // 2
        arrived(2, station)
        arrived(2, OWN + station)
        correlate(1, 2, station, False)
        packed[7 * OWN + station] = stage[...].astype(BF16)
        far_copy(station).start()
        return carry

    def last_pairs(k, carry):
        n = lax.rem(k, 2)
        station = lax.rem(HALF + k // 2 + HALF * n, OWN)
        slot = 3 - 2 * n
        arrived(slot, station)
        arrived(slot, OWN + station)
        swapped_pairs(n, station)
        neighbour_pairs(n, station)
        return carry

    def far_own_pairs(station, carry):
        unit = 2 * OWN + station
        correlate(0, 2, station, False)
        packed[unit] = stage[...].astype(BF16)
        out_copy(unit, far, station).start()
        return carry

    lax.fori_loop(0, 2 * HALF, first_swaps, 0)
    lax.fori_loop(0, OWN, far_pairs, 0)
    lax.fori_loop(0, 2 * HALF, last_pairs, 0)
    lax.fori_loop(0, OWN, far_own_pairs, 0)

    def land_far_pairs(station, carry):
        far_copy(station).wait_recv()
        far_out(station).start()
        return carry

    def land_swaps(k, carry):
        n = lax.rem(k, 2)
        station = lax.rem(k // 2 + HALF * n, OWN)
        swap_copy(n, station).wait_recv()
        swap_out(n, station).start()
        return carry

    lax.fori_loop(0, OWN, land_far_pairs, 0)
    lax.fori_loop(0, 2 * OWN, land_swaps, 0)

    def finish(station, carry):
        for n in range(2):
            swap_copy(n, station).wait_send()
            swap_out(n, station).wait()
        far_copy(station).wait_send()
        far_out(station).wait()
        for slot in range(5):
            out_copy(slot * OWN + station, peers[slot], station).wait()
        for pol in range(POL):
            for way in (UP, DOWN, PAIR):
                chunk_copy(pol * OWN + station, way).wait_send()
        return carry

    lax.fori_loop(0, OWN, finish, 0)
    for pol in range(POL):
        for n in range(HALF):
            forward_up(pol, n).wait_send()
            forward_down(pol, n).wait_send()
    for step in steps:
        dish_copy(0, step).wait_send()
        dish_copy(1, step).wait_send()
        weight_copy(step).wait_send()
    for step in range(1, CHAN):
        power_copy(step).wait_send()
    for copy in inverse_copies:
        copy.wait_send()

    @pl.when(half == 0)
    def _():
        for pol in range(POL):
            halo_copy(pol).wait_send()


def widen(narrow_hbm, wide_hbm, narrow, wide, in_sem, out_sem):
    size = narrow.shape[0] // WIDEN_STEPS
    pieces = [pl.ds(step * size, size) for step in range(WIDEN_STEPS)]
    loads = [
        pltpu.make_async_copy(narrow_hbm.at[piece], narrow.at[piece], in_sem.at[step])
        for step, piece in enumerate(pieces)
    ]
    stores = [
        pltpu.make_async_copy(wide.at[piece], wide_hbm.at[piece], out_sem.at[step])
        for step, piece in enumerate(pieces)
    ]
    for load in loads:
        load.start()
    for piece, load, store in zip(pieces, loads, stores):
        load.wait()
        wide[piece] = narrow[piece].astype(F32)
        store.start()
    for store in stores:
        store.wait()


def widened(array):
    shape = array.shape
    flat = array.reshape(-1, LANES)
    hbm = pl.BlockSpec(memory_space=pltpu.HBM)
    wide = pl.pallas_call(
        widen,
        out_shape=jax.ShapeDtypeStruct(flat.shape, F32),
        in_specs=[hbm],
        out_specs=hbm,
        scratch_shapes=[
            pltpu.VMEM(flat.shape, BF16), pltpu.VMEM(flat.shape, F32),
            pltpu.SemaphoreType.DMA((WIDEN_STEPS,)), pltpu.SemaphoreType.DMA((WIDEN_STEPS,)),
        ],
        compiler_params=pltpu.CompilerParams(vmem_limit_bytes=WIDEN_GRANT),
    )(flat)
    return wide.reshape(shape)


def per_device(voltages, fir_taps, station_map, beam_index, weight_table):
    parts, _, dishes, frames, pols, fine = voltages.shape
    rows = voltages.reshape(parts, dishes, frames, pols, NT, LANES)
    rows = rows.swapaxes(3, 4).reshape(parts, dishes, frames * NT * pols, LANES)
    table = jnp.asarray(dft_table(), BF16)
    weights = jnp.transpose(weight_table[:, :, 0, :], (0, 2, 1))
    hbm = pl.BlockSpec(memory_space=pltpu.HBM)
    dma = pltpu.SemaphoreType.DMA
    chunk = (FRAMES * BEAMS, 2 * FINE)
    operands = (
        station_map[None], beam_index[None], weights, rows, fir_taps, table,
    )
    result = pl.pallas_call(
        kernel,
        out_shape=jax.ShapeDtypeStruct((2, OWN, STN * OWN, 8 * BEAMS, LANES), BF16),
        in_specs=[hbm] * len(operands),
        out_specs=hbm,
        scratch_shapes=[
            *(pltpu.VMEM(a.shape, a.dtype) for a in operands),
            pltpu.VMEM((1, dishes), jnp.int32),
            pltpu.SMEM((1, dishes), jnp.int32),
            pltpu.VMEM((STN, 2 * SHARE, LANES), BF16),
            pltpu.VMEM((2 * SHARE * PITCH, LANES), F32),
            pltpu.VMEM((STN - 1, POL, 2 * SHARE, FRAMES * FINE), BF16),
            pltpu.VMEM((POL, STN * 2 * SHARE, FRAMES * FINE), BF16),
            pltpu.VMEM((STN * 2 * SHARE, LANES), BF16),
            pltpu.VMEM((2 * OWN * BEAMS, STN * 2 * SHARE), BF16),
            pltpu.VMEM((POL, 2 * OWN, (HISTORY + FRAMES) * BEAMS, FINE), F32),
            pltpu.VMEM((OWN * FRAMES * BEAMS, 2 * FINE), BF16),
            pltpu.VMEM((5, POL * OWN, *chunk), BF16),
            pltpu.VMEM((2, OWN * POL, *chunk), F32),
            pltpu.VMEM((2, OWN, 8 * BEAMS, LANES), F32),
            pltpu.VMEM((8 * OWN, 2, OWN, 8 * BEAMS, LANES), BF16),
            pltpu.VMEM((2, OWN, 2, OWN, 8 * BEAMS, LANES), BF16),
            pltpu.VMEM((OWN, 2, OWN, 8 * BEAMS, LANES), BF16),
            pltpu.VMEM((BEAMS, LANES), F32),
            pltpu.VMEM((CHAN - 1, BEAMS, LANES), F32),
            pltpu.VMEM((5, BEAMS, LANES), F32),
            dma((POL, STN - 1)), dma((POL, STN - 1)),
            dma((STN - 1,)), dma((STN - 1,)),
            dma((POL,)), dma((POL,)),
            dma((3, POL * OWN)), dma((5, POL * OWN)), dma((2, POL, HALF)),
            dma((CHAN - 1,)), dma((CHAN - 1,)),
            dma((5,)), dma((5,)),
            dma((5 * OWN,)),
            dma((2, OWN)), dma((2, OWN)),
            dma((OWN,)), dma((OWN,)),
            dma((len(operands),)), dma,
        ],
        compiler_params=pltpu.CompilerParams(
            collective_id=0, has_side_effects=True, vmem_limit_bytes=VMEM_GRANT
        ),
    )(*operands)
    result = widened(result).reshape(2, OWN, STN * OWN, BEAMS, POL, NT, POL, LANES)
    result = result.swapaxes(5, 6).reshape(2, 1, OWN, STN * OWN, BEAMS, POL, POL, fine)
    return result[None]


def solution(mesh):
    in_specs = (
        P(None, "chan", "stn", "tm", None, None),
        P(),
        P("stn"),
        P("stn"),
        P(None, None, "chan", None),
    )
    out_specs = P("tm", None, "chan", "stn", None, None, None, None, None)
    return jax.shard_map(
        per_device, mesh=mesh, in_specs=in_specs, out_specs=out_specs, check_vma=False
    )
```

```python
import functools

import jax
import jax.numpy as jnp
import numpy as np
from jax import lax
from jax.experimental import pallas as pl
from jax.experimental.pallas import tpu as pltpu
from jax.sharding import PartitionSpec as P

MESH = pl.DeviceIdType.MESH
F32 = jnp.float32
BF16 = jnp.bfloat16
EPSILON = 1e-06
STN = 8
RING = 4
CHAN = 8
SHARE = 8
OWN = 4
HALF = OWN // 2
BEAMS = 8
POL = 2
FRAMES = 16
TAPS = 16
FINE = 256
LANES = 128
NT = FINE // LANES
HISTORY = TAPS - 1
VMEM_GRANT = 67043328 - 4 * 1024 * 1024
PITCH = 72
DENOMINATOR = float(CHAN * FRAMES * FINE)


WIDEN_STEPS = 16
WIDEN_GRANT = 62 * 1024 * 1024
ROUTE = ((1, 2), (1, 1), (1, 3), (1, 0), (0, 2), (0, 1), (0, 3))
SECOND = (3, 2, 1, 0, 6, 5, 4)


def dft_table():
    step = np.arange(FINE)
    angle = (step[:, None] * step[None, :] % FINE) * (2.0 * np.pi / FINE)
    cosine, sine = np.cos(angle), np.sin(angle)
    return np.block([[cosine, -sine], [sine, cosine]]).astype(np.float32)


def kernel(
    map_hbm, row_hbm, table_hbm, v_hbm, taps_hbm, tab_hbm, out_ref,
    map_ref, row_ref, table_ref, v_ref, taps_ref, tab_ref, perm_vec, perm_ref, wt_ref, regroup, send_v, recv_v, recv_wt, weights, beams, filtered, formed, scaled, stage, packed, land_swap, land_far,
    power, power_all, inverse,
    a_send, a_recv, w_send, w_recv, h_send, h_recv, g_send, g_recv, f_send,
    p_send, p_recv, i_send, i_recv, o_sem, x_send, x_recv, y_send, y_recv, load_sem, perm_sem,
):
    half = lax.axis_index("tm")
    me = lax.axis_index("stn")
    chan = lax.axis_index("chan")
    row, col = me // RING, me % RING
    up = row * RING + lax.rem(col + 1, RING)
    down = row * RING + lax.rem(col + 3, RING)
    far = row * RING + lax.rem(col + 2, RING)
    pair = (1 - row) * RING + col
    peers = {0: me, 1: up, 2: far, 3: down, 4: pair}

    def remote(src, dst, send, recv, **where):
        return pltpu.make_async_remote_copy(
            src_ref=src, dst_ref=dst, send_sem=send, recv_sem=recv,
            device_id=where, device_id_type=MESH,
        )

    barrier = pltpu.get_barrier_semaphore()
    pl.semaphore_signal(barrier, inc=1, device_id={"tm": 1 - half}, device_id_type=MESH)
    for step in range(1, STN):
        pl.semaphore_signal(
            barrier, inc=1, device_id={"stn": lax.rem(me + step, STN)}, device_id_type=MESH
        )
    for step in range(1, CHAN):
        pl.semaphore_signal(
            barrier, inc=1, device_id={"chan": lax.rem(chan + step, CHAN)}, device_id_type=MESH
        )

    loads = [
        pltpu.make_async_copy(source, target, load_sem.at[k])
        for k, (source, target) in enumerate(
            (
                (map_hbm, map_ref), (row_hbm, row_ref), (table_hbm, table_ref),
                (v_hbm, v_ref), (taps_hbm, taps_ref), (tab_hbm, tab_ref),
            )
        )
    ]
    for load in loads:
        load.start()
    loads[0].wait()
    loads[1].wait()

    dishes = STN * SHARE
    line_id = lax.broadcasted_iota(jnp.int32, (dishes, dishes), 0)
    column_id = lax.broadcasted_iota(jnp.int32, (dishes, dishes), 1)

    def over_lanes(mask, value):
        return jnp.sum(jnp.where(mask, value, 0), axis=1, keepdims=True, dtype=jnp.int32)

    def over_lines(mask, value):
        return jnp.sum(jnp.where(mask, value, 0), axis=0, keepdims=True, dtype=jnp.int32)

    station_all = jnp.broadcast_to(map_ref[...], (dishes, dishes))
    row_all = jnp.broadcast_to(row_ref[...], (dishes, dishes))
    holder_across = station_all // OWN
    holder_line = over_lanes(line_id == column_id, holder_across)
    holder_down = jnp.broadcast_to(holder_line, (dishes, dishes))
    same = holder_across == holder_down
    rank_down = over_lanes(same & (column_id < line_id), 1)
    slot_down = holder_down * SHARE + rank_down
    perm_vec[...] = over_lines(slot_down == column_id, line_id)
    perm_copy = pltpu.make_async_copy(perm_vec, perm_ref, perm_sem)
    perm_copy.start()
    rank_across = over_lines(same & (line_id < column_id), 1)
    hot = holder_across * SHARE + rank_across == line_id
    station_slot = over_lanes(hot, station_all % OWN)
    row_slot = over_lanes(hot, row_all)

    loads[2].wait()
    rows = table_ref.shape[2]
    weight_re, weight_im = table_ref[0].astype(F32), table_ref[1].astype(F32)
    blank = jnp.zeros((LANES - 2 * OWN * BEAMS, rows), F32)
    row_hot = (row_slot == lax.broadcasted_iota(jnp.int32, (dishes, rows), 1)).astype(F32)
    lane_station = lax.broadcasted_iota(jnp.int32, (dishes, LANES), 1) // BEAMS % OWN
    chosen = []
    for first, second in ((weight_re, weight_im), (-weight_im, weight_re)):
        spread = jnp.concatenate([first] * OWN + [second] * OWN + [blank], axis=0)
        value = lax.dot_general(
            row_hot.astype(BF16), spread.astype(BF16), (((1,), (1,)), ((), ())),
            preferred_element_type=F32,
        )
        chosen.append(jnp.where(lane_station == station_slot, value, 0.0))
    for holder in range(STN):
        lines = slice(holder * SHARE, (holder + 1) * SHARE)
        wt_ref[holder] = jnp.concatenate([part[lines] for part in chosen], axis=0).astype(BF16)
    loads[3].wait()
    perm_copy.wait()

    def regrouped(holder, store):
        for part in range(2):
            for e in range(SHARE):
                dish = perm_ref[0, holder * SHARE + e]
                line = (part * SHARE + e) * PITCH
                regroup[line : line + FRAMES * NT * POL, :] = v_ref[part, dish].astype(F32)
        for pol in range(POL):
            for tile in range(FRAMES * NT):
                value = regroup[pl.ds(tile * POL + pol, 2 * SHARE, stride=PITCH), :]
                store(pol, tile * LANES, value.astype(BF16))

    mine = pl.ds(pl.multiple_of(me * 2 * SHARE, 2 * SHARE), 2 * SHARE)

    def holder_at(step):
        rows_away, ring_away = ROUTE[step]
        return (1 - row if rows_away else row) * RING + lax.rem(col + ring_away, RING)

    def dish_copy(pol, step):
        return remote(
            send_v.at[step, pol], recv_v.at[pol, mine],
            a_send.at[pol, step], a_recv.at[pol, step], stn=holder_at(step),
        )

    def weight_copy(step):
        holder = holder_at(step)
        return remote(
            wt_ref.at[holder], recv_wt.at[mine], w_send.at[step], w_recv.at[step], stn=holder
        )

    def prepare(step):
        def store(pol, lane, value):
            send_v[step, pol, :, lane : lane + LANES] = value

        regrouped(holder_at(step), store)

    steps = range(STN - 1)
    prepare(0)
    prepare(1)
    pl.semaphore_wait(barrier, 1 + (STN - 1) + (CHAN - 1))
    for step in steps:
        if step >= 2:
            prepare(step)
        if step >= 1:
            dish_copy(0, step - 1).start()

    def store_own(pol, lane, value):
        recv_v[pol, mine, lane : lane + LANES] = value

    regrouped(me, store_own)
    dish_copy(0, STN - 2).start()
    for step in steps:
        weight_copy(step).start()
    for step in SECOND:
        dish_copy(1, step).start()
    recv_wt[mine, :] = wt_ref[me]
    power[...] = jnp.zeros_like(power)
    lane_id = lax.broadcasted_iota(jnp.int32, (BEAMS, LANES), 1)

    for step in steps:
        weight_copy(step).wait_recv()
    weights[...] = jnp.transpose(recv_wt[...].astype(F32))[: 2 * OWN * BEAMS, :].astype(BF16)

    def halo_copy(pol):
        return remote(
            beams.at[pol, :, pl.ds((HISTORY + 1) * BEAMS, HISTORY * BEAMS), :],
            beams.at[pol, :, pl.ds(0, HISTORY * BEAMS), :],
            h_send.at[pol], h_recv.at[pol], tm=1 - half,
        )

    def chunk_copy(chunk, way):
        slot, target = ((3, up), (1, down), (4, pair))[way]
        return remote(
            formed.at[0, chunk], formed.at[slot, chunk],
            g_send.at[way, chunk], g_recv.at[slot, chunk], stn=target,
        )

    loads[4].wait()
    loads[5].wait()
    UP, DOWN, PAIR = range(3)

    def send_first(station, carry):
        chunk_copy(station, UP).start()
        chunk_copy(lax.rem(station + HALF, OWN), DOWN).start()
        chunk_copy(station, PAIR).start()
        return carry

    for pol in range(POL):
        for step in steps:
            dish_copy(pol, step).wait_recv()

        def steer(frame, carry):
            lanes = pl.ds(pl.multiple_of(frame * FINE, FINE), FINE)
            value = jnp.dot(weights[...], recv_v[pol, :, lanes], preferred_element_type=F32)
            line = pl.ds(pl.multiple_of((HISTORY + frame) * BEAMS, BEAMS), BEAMS)
            for j in range(2 * OWN):
                beams[pol, j, line, :] = value[j * BEAMS : (j + 1) * BEAMS, :]
            return carry

        lax.fori_loop(0, FRAMES, steer, 0)

        @pl.when(half == 0)
        def _():
            beams[pol, :, : HISTORY * BEAMS, :] = jnp.zeros((2 * OWN, HISTORY * BEAMS, FINE), F32)
            halo_copy(pol).start()

        @pl.when(half == 1)
        def _():
            halo_copy(pol).wait_recv()

        def filter_station(station, carry):
            for part in range(2):
                for tile in range(NT):
                    lanes = slice(tile * LANES, (tile + 1) * LANES)
                    taps = [
                        jnp.broadcast_to(taps_ref[j : j + 1, lanes], (BEAMS, LANES))
                        for j in range(TAPS)
                    ]
                    outs = []
                    for frame in range(FRAMES):
                        total = None
                        for j in range(TAPS):
                            line = (frame + HISTORY - j) * BEAMS
                            term = taps[j] * beams[
                                pol, part * OWN + station, line : line + BEAMS, lanes
                            ]
                            total = term if total is None else total + term
                        outs.append(total)
                        if frame % 2:
                            base = pl.multiple_of(
                                station * FRAMES * BEAMS + (frame - 1) * BEAMS, 2 * BEAMS
                            )
                            lane = part * FINE + tile * LANES
                            filtered[pl.ds(base, 2 * BEAMS), lane : lane + LANES] = (
                                jnp.concatenate(outs, axis=0).astype(BF16)
                            )
                            outs = []
            return carry

        lax.fori_loop(0, OWN, filter_station, 0)

        def transform(station, carry):
            lines = pl.ds(pl.multiple_of(station * FRAMES * BEAMS, FRAMES * BEAMS), FRAMES * BEAMS)
            value = jnp.dot(filtered[lines, :], tab_ref[...], preferred_element_type=F32)
            formed[0, pol * OWN + station] = value.astype(BF16)
            squares = jnp.sum((value * value).reshape(FRAMES, BEAMS, 2 * FINE), axis=0)
            squares = sum(squares[:, k * LANES : (k + 1) * LANES] for k in range(4))
            total = jnp.sum(squares, axis=1, keepdims=True)
            power[...] += jnp.where(lane_id == station * POL + pol, total, 0.0)
            return carry

        lax.fori_loop(0, OWN, transform, 0)

        if pol == 0:
            lax.fori_loop(0, OWN, send_first, 0)

    def arrived(slot, chunk):
        remote(
            formed.at[slot, chunk], formed.at[slot, chunk], g_send.at[0, chunk],
            g_recv.at[slot, chunk], stn=up,
        ).wait_recv()

    def forward_up(pol, n):
        chunk = pol * OWN + n
        return remote(
            formed.at[3, chunk], formed.at[2, chunk],
            f_send.at[0, pol, n], g_recv.at[2, chunk], stn=up,
        )

    def forward_down(pol, n):
        chunk = pol * OWN + HALF + n
        return remote(
            formed.at[1, chunk], formed.at[2, chunk],
            f_send.at[1, pol, n], g_recv.at[2, chunk], stn=down,
        )

    def power_copy(step):
        return remote(
            power, power_all.at[step - 1], p_send.at[step - 1], p_recv.at[step - 1],
            chan=lax.rem(chan + step, CHAN),
        )

    for step in range(1, CHAN):
        power_copy(step).start()

    def send_second(n, carry):
        chunk_copy(OWN + n, UP).start()
        chunk_copy(OWN + HALF + n, DOWN).start()
        chunk_copy(OWN + 2 * n, PAIR).start()
        chunk_copy(OWN + 2 * n + 1, PAIR).start()
        arrived(3, n)
        forward_up(0, n).start()
        arrived(1, HALF + n)
        forward_down(0, n).start()
        return carry

    lax.fori_loop(0, HALF, send_second, 0)
    for step in range(1, CHAN):
        power_copy(step).wait_recv()
    total = power[...]
    for step in range(1, CHAN):
        total = total + power_all[step - 1]
    inverse[0] = lax.rsqrt(total / DENOMINATOR + EPSILON)
    inverse_copies = [
        remote(inverse.at[0], inverse.at[slot], i_send.at[slot], i_recv.at[slot], stn=target)
        for slot, target in ((1, down), (2, far), (3, up), (4, pair))
    ]

    def lane_of(slot, index):
        tile = inverse[slot]
        one = jnp.sum(jnp.where(lane_id == index, tile, 0.0), axis=1, keepdims=True)
        return jnp.broadcast_to(one, (BEAMS, LANES))

    def scale_chunk(which, slot, station):
        for pol in range(POL):
            factor = lane_of(slot, station * POL + pol) * (1.0 / FRAMES)
            for pairs in range(FRAMES // 2):
                lines = slice(pairs * 2 * BEAMS, (pairs + 1) * 2 * BEAMS)
                for tile in range(4):
                    lanes = slice(tile * LANES, (tile + 1) * LANES)
                    value = formed[slot, pol * OWN + station, lines, lanes].astype(F32)
                    scaled[which, station * POL + pol, lines, lanes] = jnp.concatenate(
                        [value[:BEAMS] * factor, value[BEAMS:] * factor], axis=0
                    )

    def correlate(which, slot, station, swapped):
        for q in range(POL):
            factor = lane_of(slot, station * POL + q)
            for tile in range(NT):
                re_lanes = slice(tile * LANES, (tile + 1) * LANES)
                im_lanes = slice(FINE + tile * LANES, FINE + (tile + 1) * LANES)
                real = [None] * (OWN * POL)
                imag = [None] * (OWN * POL)
                for pairs in range(FRAMES // 2):
                    lines = slice(pairs * 2 * BEAMS, (pairs + 1) * 2 * BEAMS)
                    right_re = formed[slot, q * OWN + station, lines, re_lanes].astype(F32)
                    right_im = formed[slot, q * OWN + station, lines, im_lanes].astype(F32)
                    for part in range(2):
                        cr = right_re[part * BEAMS : (part + 1) * BEAMS]
                        ci = right_im[part * BEAMS : (part + 1) * BEAMS]
                        line = (pairs * 2 + part) * BEAMS
                        for c in range(OWN * POL):
                            ar = scaled[which, c, line : line + BEAMS, re_lanes]
                            ai = scaled[which, c, line : line + BEAMS, im_lanes]
                            re = ar * cr + ai * ci
                            im = ar * ci - ai * cr if swapped else ai * cr - ar * ci
                            real[c] = re if real[c] is None else real[c] + re
                            imag[c] = im if imag[c] is None else imag[c] + im
                for c in range(OWN * POL):
                    s, p = c // POL, c % POL
                    line = q * 4 + tile * 2 + p if swapped else p * 4 + tile * 2 + q
                    lines = pl.ds(line, BEAMS, stride=8)
                    stage[0, s, lines, :] = real[c] * factor
                    stage[1, s, lines, :] = imag[c] * factor

    def out_copy(unit, block, station):
        return pltpu.make_async_copy(
            packed.at[unit], out_ref.at[:, :, block * OWN + station], o_sem.at[unit]
        )

    for copy in inverse_copies:
        copy.start()

    def own_scale(station, carry):
        scale_chunk(0, 0, station)
        return carry

    lax.fori_loop(0, OWN, own_scale, 0)

    def own_pairs(station, carry):
        correlate(0, 0, station, False)
        packed[station] = stage[...].astype(BF16)
        out_copy(station, me, station).start()
        return carry

    lax.fori_loop(0, OWN, own_pairs, 0)
    for copy in inverse_copies:
        copy.wait_recv()

    def neighbour_pairs(n, station):
        slot = 3 - 2 * n
        unit = slot * OWN + station
        correlate(0, slot, station, False)
        packed[unit] = stage[...].astype(BF16)
        out_copy(unit, row * RING + lax.rem(col + slot, RING), station).start()

    def first_pairs(k, carry):
        arrived(3, OWN + k)
        forward_up(1, k).start()
        arrived(1, OWN + HALF + k)
        forward_down(1, k).start()
        chunk_copy(OWN + HALF + k, UP).start()
        chunk_copy(OWN + k, DOWN).start()

        def near(n, c):
            neighbour_pairs(n, k + HALF * n)
            return c

        lax.fori_loop(0, 2, near, 0)

        def partner(n, c):
            station = 2 * k + n
            arrived(4, station)
            arrived(4, OWN + station)
            scale_chunk(1, 4, station)
            unit = 4 * OWN + station
            correlate(0, 4, station, False)
            packed[unit] = stage[...].astype(BF16)
            out_copy(unit, pair, station).start()
            return c

        lax.fori_loop(0, 2, partner, 0)
        return carry

    lax.fori_loop(0, HALF, first_pairs, 0)

    across = [(1 - row) * RING + lax.rem(col + step, RING) for step in range(RING)]

    def swap_copy(n, station):
        return remote(
            packed.at[5 * OWN + n * OWN + station], land_swap.at[n, station],
            x_send.at[n, station], x_recv.at[n, station],
            stn=row * RING + lax.rem(col + 3 - 2 * n, RING),
        )

    def far_copy(station):
        return remote(
            packed.at[7 * OWN + station], land_far.at[station],
            y_send.at[station], y_recv.at[station], stn=pair,
        )

    def swap_out(n, station):
        block = (1 - row) * RING + lax.rem(col + 1 + 2 * n, RING)
        stations = pl.ds(pl.multiple_of(block * OWN, OWN), OWN)
        return pltpu.make_async_copy(
            land_swap.at[n, station], out_ref.at[:, station, stations], x_recv.at[n, station]
        )

    def far_out(station):
        return pltpu.make_async_copy(
            land_far.at[station], out_ref.at[:, :, across[2] * OWN + station], y_recv.at[station]
        )

    def swapped_pairs(n, station):
        correlate(1, 3 - 2 * n, station, True)
        packed[5 * OWN + n * OWN + station] = stage[...].astype(BF16)
        swap_copy(n, station).start()

    def first_swaps(k, carry):
        n = lax.rem(k, 2)
        swapped_pairs(n, k // 2 + HALF * n)
        return carry

    def far_pairs(k, carry):
        station = lax.rem(k, 2) * HALF + k // 2
        arrived(2, station)
        arrived(2, OWN + station)
        correlate(1, 2, station, False)
        packed[7 * OWN + station] = stage[...].astype(BF16)
        far_copy(station).start()
        return carry

    def last_pairs(k, carry):
        n = lax.rem(k, 2)
        station = lax.rem(HALF + k // 2 + HALF * n, OWN)
        slot = 3 - 2 * n
        arrived(slot, station)
        arrived(slot, OWN + station)
        swapped_pairs(n, station)
        neighbour_pairs(n, station)
        return carry

    def far_own_pairs(station, carry):
        unit = 2 * OWN + station
        correlate(0, 2, station, False)
        packed[unit] = stage[...].astype(BF16)
        out_copy(unit, far, station).start()
        return carry

    lax.fori_loop(0, 2 * HALF, first_swaps, 0)
    lax.fori_loop(0, OWN, far_pairs, 0)
    lax.fori_loop(0, 2 * HALF, last_pairs, 0)
    lax.fori_loop(0, OWN, far_own_pairs, 0)

    def land_far_pairs(station, carry):
        far_copy(station).wait_recv()
        far_out(station).start()
        return carry

    def land_swaps(k, carry):
        n = lax.rem(k, 2)
        station = lax.rem(k // 2 + HALF * n, OWN)
        swap_copy(n, station).wait_recv()
        swap_out(n, station).start()
        return carry

    lax.fori_loop(0, OWN, land_far_pairs, 0)
    lax.fori_loop(0, 2 * OWN, land_swaps, 0)

    def finish(station, carry):
        for n in range(2):
            swap_copy(n, station).wait_send()
            swap_out(n, station).wait()
        far_copy(station).wait_send()
        far_out(station).wait()
        for slot in range(5):
            out_copy(slot * OWN + station, peers[slot], station).wait()
        for pol in range(POL):
            for way in (UP, DOWN, PAIR):
                chunk_copy(pol * OWN + station, way).wait_send()
        return carry

    lax.fori_loop(0, OWN, finish, 0)
    for pol in range(POL):
        for n in range(HALF):
            forward_up(pol, n).wait_send()
            forward_down(pol, n).wait_send()
    for step in steps:
        dish_copy(0, step).wait_send()
        dish_copy(1, step).wait_send()
        weight_copy(step).wait_send()
    for step in range(1, CHAN):
        power_copy(step).wait_send()
    for copy in inverse_copies:
        copy.wait_send()

    @pl.when(half == 0)
    def _():
        for pol in range(POL):
            halo_copy(pol).wait_send()


def widen(narrow_hbm, wide_hbm, narrow, wide, in_sem, out_sem):
    size = narrow.shape[0] // WIDEN_STEPS
    pieces = [pl.ds(step * size, size) for step in range(WIDEN_STEPS)]
    loads = [
        pltpu.make_async_copy(narrow_hbm.at[piece], narrow.at[piece], in_sem.at[step])
        for step, piece in enumerate(pieces)
    ]
    stores = [
        pltpu.make_async_copy(wide.at[piece], wide_hbm.at[piece], out_sem.at[step])
        for step, piece in enumerate(pieces)
    ]
    for load in loads:
        load.start()
    for piece, load, store in zip(pieces, loads, stores):
        load.wait()
        wide[piece] = narrow[piece].astype(F32)
        store.start()
    for store in stores:
        store.wait()


def widened(array):
    shape = array.shape
    flat = array.reshape(-1, LANES)
    hbm = pl.BlockSpec(memory_space=pltpu.HBM)
    wide = pl.pallas_call(
        widen,
        out_shape=jax.ShapeDtypeStruct(flat.shape, F32),
        in_specs=[hbm],
        out_specs=hbm,
        scratch_shapes=[
            pltpu.VMEM(flat.shape, BF16), pltpu.VMEM(flat.shape, F32),
            pltpu.SemaphoreType.DMA((WIDEN_STEPS,)), pltpu.SemaphoreType.DMA((WIDEN_STEPS,)),
        ],
        compiler_params=pltpu.CompilerParams(vmem_limit_bytes=WIDEN_GRANT),
    )(flat)
    return wide.reshape(shape)


def per_device(voltages, fir_taps, station_map, beam_index, weight_table):
    parts, _, dishes, frames, pols, fine = voltages.shape
    rows = voltages.reshape(parts, dishes, frames, pols, NT, LANES)
    rows = rows.swapaxes(3, 4).reshape(parts, dishes, frames * NT * pols, LANES)
    table = jnp.asarray(dft_table(), BF16)
    weights = jnp.transpose(weight_table[:, :, 0, :], (0, 2, 1))
    hbm = pl.BlockSpec(memory_space=pltpu.HBM)
    dma = pltpu.SemaphoreType.DMA
    chunk = (FRAMES * BEAMS, 2 * FINE)
    operands = (
        station_map[None], beam_index[None], weights, rows, fir_taps, table,
    )
    result = pl.pallas_call(
        kernel,
        out_shape=jax.ShapeDtypeStruct((2, OWN, STN * OWN, 8 * BEAMS, LANES), BF16),
        in_specs=[hbm] * len(operands),
        out_specs=hbm,
        scratch_shapes=[
            *(pltpu.VMEM(a.shape, a.dtype) for a in operands),
            pltpu.VMEM((1, dishes), jnp.int32),
            pltpu.SMEM((1, dishes), jnp.int32),
            pltpu.VMEM((STN, 2 * SHARE, LANES), BF16),
            pltpu.VMEM((2 * SHARE * PITCH, LANES), F32),
            pltpu.VMEM((STN - 1, POL, 2 * SHARE, FRAMES * FINE), BF16),
            pltpu.VMEM((POL, STN * 2 * SHARE, FRAMES * FINE), BF16),
            pltpu.VMEM((STN * 2 * SHARE, LANES), BF16),
            pltpu.VMEM((2 * OWN * BEAMS, STN * 2 * SHARE), BF16),
            pltpu.VMEM((POL, 2 * OWN, (HISTORY + FRAMES) * BEAMS, FINE), F32),
            pltpu.VMEM((OWN * FRAMES * BEAMS, 2 * FINE), BF16),
            pltpu.VMEM((5, POL * OWN, *chunk), BF16),
            pltpu.VMEM((2, OWN * POL, *chunk), F32),
            pltpu.VMEM((2, OWN, 8 * BEAMS, LANES), F32),
            pltpu.VMEM((8 * OWN, 2, OWN, 8 * BEAMS, LANES), BF16),
            pltpu.VMEM((2, OWN, 2, OWN, 8 * BEAMS, LANES), BF16),
            pltpu.VMEM((OWN, 2, OWN, 8 * BEAMS, LANES), BF16),
            pltpu.VMEM((BEAMS, LANES), F32),
            pltpu.VMEM((CHAN - 1, BEAMS, LANES), F32),
            pltpu.VMEM((5, BEAMS, LANES), F32),
            dma((POL, STN - 1)), dma((POL, STN - 1)),
            dma((STN - 1,)), dma((STN - 1,)),
            dma((POL,)), dma((POL,)),
            dma((3, POL * OWN)), dma((5, POL * OWN)), dma((2, POL, HALF)),
            dma((CHAN - 1,)), dma((CHAN - 1,)),
            dma((5,)), dma((5,)),
            dma((5 * OWN,)),
            dma((2, OWN)), dma((2, OWN)),
            dma((OWN,)), dma((OWN,)),
            dma((len(operands),)), dma,
        ],
        compiler_params=pltpu.CompilerParams(
            collective_id=0, has_side_effects=True, vmem_limit_bytes=VMEM_GRANT
        ),
    )(*operands)
    result = widened(result).reshape(2, OWN, STN * OWN, BEAMS, POL, NT, POL, LANES)
    result = result.swapaxes(5, 6).reshape(2, 1, OWN, STN * OWN, BEAMS, POL, POL, fine)
    return result[None]


def solution(mesh):
    in_specs = (
        P(None, "chan", "stn", "tm", None, None),
        P(),
        P("stn"),
        P("stn"),
        P(None, None, "chan", None),
    )
    out_specs = P("tm", None, "chan", "stn", None, None, None, None, None)
    return jax.shard_map(
        per_device, mesh=mesh, in_specs=in_specs, out_specs=out_specs, check_vma=False
    )
```
